64 devices in a mesh: dp: 4 (over x, y), ep: 16 (over z, core).
Axes of the slice: x: 2, y: 2, z: 8, core: 2. Of those that a mesh axis runs over, the one named last changes fastest.
The devices are a block of a 4x4x8 slice.
Arguments:
- tokens: bfloat16 [16384, 2048], P(('dp', 'ep')), parts along dimension 0
- expert_ids: int32 [16384, 8], P(('dp', 'ep')), parts along dimension 0
- gate_vals: float32 [16384, 8], P(('dp', 'ep')), parts along dimension 0
- w_gate: bfloat16 [128, 2048, 768], P('ep')
- w_up: bfloat16 [128, 2048, 768], P('ep')
- w_down: bfloat16 [128, 768, 2048], P('ep')
Outputs:
- output: bfloat16 [16384, 2048], P(('dp', 'ep')), parts along dimension 0
There are 4 independent parts. The reference program is written for one: setup_inputs(seed, part) draws one part's arguments, and reference() takes and returns one part's arrays. A program takes and returns all parts, laid end to end along the dimension named above; an argument that names none is the same for every part.
All inputs are finite; a program needn't handle non-finite values.
Results may differ from the reference program's by a relative error of at most 0.0063075.
Values are sent between devices in bfloat16 or wider.
A program may use at most 768 MiB of HBM per device.

```python
import jax
import jax.numpy as jnp
from jax import lax

D_MODEL = 2048
FFN_DIM = 768
NUM_EXPERTS = 128
TOP_K = 8
GROUP = 16
TOK_DEV = 256

DEV_LIMIT = TOP_K // 2
LOCAL_EXPERTS = NUM_EXPERTS // GROUP
PAIR_CAP = TOK_DEV * DEV_LIMIT // GROUP
EXPERT_CAP = TOK_DEV * TOP_K * GROUP // NUM_EXPERTS
TOKENS = GROUP * TOK_DEV


def perm_rows(rand_key, row_count, perm_size):
    return jax.vmap(lambda sub_key: jax.random.permutation(sub_key, perm_size))(jax.random.split(rand_key, row_count))


def draw_routing(rand_key):
    key_src, key_dst, key_slot = jax.random.split(rand_key, 3)
    src_perm = perm_rows(key_src, GROUP, GROUP)
    dst_perm = perm_rows(key_dst, GROUP, LOCAL_EXPERTS)
    flat_pos = jnp.arange(TOK_DEV)[:, None] * DEV_LIMIT + jnp.arange(DEV_LIMIT)[None, :]
    dest_dev = src_perm[:, flat_pos % GROUP]
    recv_row = jnp.arange(GROUP)[:, None, None] * PAIR_CAP + (flat_pos // GROUP)[None, :, :]
    first_loc = dst_perm[dest_dev, (2 * recv_row) % LOCAL_EXPERTS]
    second_loc = dst_perm[dest_dev, (2 * recv_row + 1) % LOCAL_EXPERTS]
    pair_ids = jnp.stack([first_loc, second_loc], axis=-1) + dest_dev[..., None] * LOCAL_EXPERTS
    ordered = pair_ids.reshape(TOKENS, TOP_K)
    scores = jax.random.randint(key_slot, (TOKENS, TOP_K), 0, 1 << 20) * TOP_K + jnp.arange(TOP_K)[None, :]
    slot_order = jnp.argsort(scores, axis=1)
    return jnp.take_along_axis(ordered, slot_order, axis=1).astype(jnp.int32)


def setup_inputs(seed: int = 0, part: int = 0) -> dict:
    base_key = jax.random.key(seed)
    key_x, key_route, key_gate = jax.random.split(jax.random.fold_in(base_key, part), 3)
    key_wg, key_wu, key_wd = jax.random.split(jax.random.key(seed + 1), 3)
    in_scale = D_MODEL ** -0.5
    out_scale = 2.0 * FFN_DIM ** -0.5
    tokens = jax.random.normal(key_x, (TOKENS, D_MODEL), jnp.float32).astype(jnp.bfloat16)
    expert_ids = draw_routing(key_route)
    logits = 1.5 * jax.random.normal(key_gate, (TOKENS, TOP_K), jnp.float32)
    gate_vals = jax.nn.softmax(logits, axis=-1)
    w_gate = (in_scale * jax.random.normal(key_wg, (NUM_EXPERTS, D_MODEL, FFN_DIM), jnp.float32)).astype(jnp.bfloat16)
    w_up = (in_scale * jax.random.normal(key_wu, (NUM_EXPERTS, D_MODEL, FFN_DIM), jnp.float32)).astype(jnp.bfloat16)
    w_down = (out_scale * jax.random.normal(key_wd, (NUM_EXPERTS, FFN_DIM, D_MODEL), jnp.float32)).astype(jnp.bfloat16)
    return {'tokens': tokens, 'expert_ids': expert_ids, 'gate_vals': gate_vals, 'w_gate': w_gate, 'w_up': w_up, 'w_down': w_down}


def expert_ffn(row_in, gate_mat, up_mat, down_mat):
    gate_act = jnp.dot(row_in, gate_mat, preferred_element_type=jnp.float32)
    up_act = jnp.dot(row_in, up_mat, preferred_element_type=jnp.float32)
    hidden = (jax.nn.silu(gate_act) * up_act).astype(jnp.bfloat16)
    return jnp.dot(hidden, down_mat, preferred_element_type=jnp.float32).astype(jnp.bfloat16)


def reference(tokens, expert_ids, gate_vals, w_gate, w_up, w_down):
    pair_count = TOKENS * TOP_K
    flat_ids = expert_ids.reshape(pair_count)
    pair_index = jnp.arange(pair_count, dtype=jnp.int32)

    def one_expert(map_item):
        expert, gate_mat, up_mat, down_mat = map_item
        member = flat_ids == expert
        slot_pos = jnp.where(member, jnp.cumsum(member.astype(jnp.int32)) - 1, EXPERT_CAP)
        pair_list = jnp.full((EXPERT_CAP,), pair_count, jnp.int32).at[slot_pos].set(pair_index, mode='drop')
        row_in = tokens[jnp.minimum(pair_list, pair_count - 1) // TOP_K]
        return pair_list, expert_ffn(row_in, gate_mat, up_mat, down_mat)

    pair_lists, expert_rows = lax.map(one_expert, (jnp.arange(NUM_EXPERTS, dtype=jnp.int32), w_gate, w_up, w_down))
    pair_out = jnp.zeros((pair_count, D_MODEL), jnp.bfloat16).at[pair_lists.reshape(-1)].set(expert_rows.reshape(-1, D_MODEL), mode='drop')
    earlier = jnp.arange(TOP_K)[None, :] < jnp.arange(TOP_K)[:, None]

    def combine_block(blk_item):
        rows_in, ids_in, gate_in, outs_in = blk_item
        dev_of = ids_in // LOCAL_EXPERTS
        same_dev = dev_of[:, :, None] == dev_of[:, None, :]
        weights = jnp.where(same_dev, gate_in[:, None, :], 0.0)
        dev_sum = jnp.einsum('tjk,tkd->tjd', weights, outs_in.astype(jnp.float32)).astype(jnp.bfloat16)
        leader = jnp.logical_not(jnp.any(same_dev & earlier[None, :, :], axis=2))
        moe_sum = jnp.sum(jnp.where(leader[:, :, None], dev_sum.astype(jnp.float32), 0.0), axis=1)
        return (rows_in.astype(jnp.float32) + moe_sum).astype(jnp.bfloat16)

    output = lax.map(combine_block, (tokens.reshape(GROUP, TOK_DEV, D_MODEL), expert_ids.reshape(GROUP, TOK_DEV, TOP_K), gate_vals.reshape(GROUP, TOK_DEV, TOP_K), pair_out.reshape(GROUP, TOK_DEV, TOP_K, D_MODEL)))
    return output.reshape(TOKENS, D_MODEL)
```

```python
import functools

import jax
import jax.numpy as jnp
from jax import lax
from jax.experimental import pallas as pl
from jax.experimental.pallas import tpu as pltpu
from jax.sharding import PartitionSpec as P

MESH = pl.DeviceIdType.MESH
SUBS = 4
F32 = jnp.float32
BF16 = jnp.bfloat16


def dot(a, b):
    return jnp.dot(a, b, preferred_element_type=F32)


def dot_nt(a, b, precision=None):
    return lax.dot_general(a, b, (((1,), (1,)), ((), ())), precision=precision, preferred_element_type=F32)


def dot_tn(a, b):
    return lax.dot_general(a, b, (((0,), (0,)), ((), ())), preferred_element_type=F32)


def moe_kernel(groups, tok, meta_in, w_gate, w_up, w_down, out, xall, meta, rows, acc, ret, wgb, wub, wdb, xin, hid, fan, fan_t,
               slot_r, slot_c, gate_c, comb, tri, base_r, base_c, ring_s, ring_r, sib_s, sib_r, mring_s, mring_r, msib_s, msib_r,
               ret_s, ret_r, wsem, loc):
    nz = groups // 2
    half = nz // 2
    tok_dev, d_model = tok.shape
    local, _, ffn = w_gate.shape
    top_k = meta.shape[1] // 2
    cap = tok_dev * (top_k // 2) // groups
    ecap = fan.shape[0]
    sub_rows = tok_dev // SUBS
    blk = 2 * cap
    nt = min(512, d_model)
    ft = min(256, ffn)
    far = nz - 1
    split = 2 * half - 3

    me = lax.axis_index('ep')
    z = me // 2
    k = me % 2
    right = ((z + 1) % nz) * 2 + k
    left = ((z + nz - 1) % nz) * 2 + k
    sib = z * 2 + 1 - k

    def source_shift(j):
        if j == 0:
            return 0
        if j == far:
            return half
        return nz - (j + 1) // 2 if j % 2 == 1 else j // 2

    def device_at(shift, c):
        return ((z + shift) % nz) * 2 + (k if c == 0 else 1 - k)

    def remote(src, dst, ssem, rsem, dev):
        return pltpu.make_async_remote_copy(src_ref=src, dst_ref=dst, send_sem=ssem, recv_sem=rsem, device_id={'ep': dev}, device_id_type=MESH)

    def sub_ds(sub, c=0):
        return pl.ds(c * tok_dev + sub * sub_rows, sub_rows)

    def ring_copy(src, dst_j, sub, dev):
        return remote(src, xall.at[dst_j, sub_ds(sub)], ring_s.at[dst_j, sub], ring_r.at[dst_j, sub], dev)

    def sib_copy(src, j, sub):
        return remote(src, xall.at[j, sub_ds(sub, 1)], sib_s.at[j, sub], sib_r.at[j, sub], sib)

    def mring_copy(src, dst_j, dev):
        return remote(src, meta.at[dst_j, :, pl.ds(0, tok_dev)], mring_s.at[dst_j], mring_r.at[dst_j], dev)

    def msib_copy(src, j):
        return remote(src, meta.at[j, :, pl.ds(tok_dev, tok_dev)], msib_s.at[j], msib_r.at[j], sib)

    def ret_copy(j, c):
        off = j * blk + c * cap
        return remote(rows.at[pl.ds(off, cap)], ret.at[pl.ds(off, cap)], ret_s.at[j, c], ret_r.at[j, c], device_at(source_shift(j), c))

    def weight_copies(expert, slot):
        return (pltpu.make_async_copy(w_gate.at[expert], wgb.at[slot], wsem.at[slot, 0]),
                pltpu.make_async_copy(w_up.at[expert], wub.at[slot], wsem.at[slot, 1]),
                pltpu.make_async_copy(w_down.at[expert], wdb.at[slot], wsem.at[slot, 2]))

    own_tok = pltpu.make_async_copy(tok, xall.at[0, pl.ds(0, tok_dev)], loc.at[0])
    own_meta = pltpu.make_async_copy(meta_in, meta.at[0, :, pl.ds(0, tok_dev)], loc.at[1])
    own_meta.start()
    own_tok.start()

    barrier = pltpu.get_barrier_semaphore()
    for step in range(1, groups):
        pl.semaphore_signal(barrier, inc=1, device_id={'ep': (me + step) % groups}, device_id_type=MESH)
    pl.semaphore_wait(barrier, groups - 1)

    mring_copy(meta_in, 1, right).start()
    mring_copy(meta_in, 2, left).start()
    msib_copy(meta_in, 0).start()
    for sub in range(SUBS):
        ring_copy(tok.at[sub_ds(sub)], 1, sub, right).start()
        ring_copy(tok.at[sub_ds(sub)], 2, sub, left).start()
    for sub in range(SUBS):
        sib_copy(tok.at[sub_ds(sub)], 0, sub).start()
    for copy in weight_copies(0, 0):
        copy.start()

    def relay_meta(j, next_j, dev):
        mring_copy(meta_in, j, dev).wait_recv()
        here = meta.at[j, :, pl.ds(0, tok_dev)]
        if next_j is not None:
            mring_copy(here, next_j, dev).start()
        msib_copy(here, j).start()

    def relay_sub(j, sub, next_j, dev):
        here = xall.at[j, sub_ds(sub)]
        ring_copy(here, j, sub, dev).wait_recv()
        if next_j is not None:
            ring_copy(here, next_j, sub, dev).start()
        sib_copy(here, j, sub).start()

    def wait_sib(j):
        msib_copy(meta.at[j, :, pl.ds(0, tok_dev)], j).wait_recv()
        for sub in range(SUBS):
            sib_copy(xall.at[j, sub_ds(sub)], j, sub).wait_recv()

    tok_row = lax.broadcasted_iota(jnp.int32, (tok_dev, tok_dev), 0)
    tok_col = lax.broadcasted_iota(jnp.int32, (tok_dev, tok_dev), 1)
    tri[...] = jnp.where(tok_row < tok_col, 1.0, 0.0).astype(BF16)

    own_meta.wait()
    row_id = lax.broadcasted_iota(jnp.int32, (2 * nz, tok_dev), 0)
    peer_lo = jnp.zeros((2 * nz, tok_dev), jnp.int32)
    for j in range(nz):
        for c in range(2):
            peer = device_at((nz - source_shift(j)) % nz, c)
            peer_lo = jnp.where(row_id == 2 * j + c, peer * local, peer_lo)
    peer_lo = peer_lo.astype(F32)
    own_ids = meta[0, 0:top_k, 0:tok_dev]
    picked = jnp.zeros((2 * nz, tok_dev), F32)
    for i in range(top_k):
        rel = own_ids[i:i + 1, :] - peer_lo
        picked = jnp.where((rel >= 0) & (rel < local), 1.0, picked)
    rank = jnp.where(picked > 0, dot(picked.astype(BF16), tri[...]), -1.0)
    cap_iota = lax.broadcasted_iota(jnp.int32, (cap, tok_dev), 0).astype(F32)
    for r in range(2 * nz):
        comb[r * cap:(r + 1) * cap, :] = jnp.where(rank[r:r + 1, :] == cap_iota, 1.0, 0.0).astype(BF16)

    lo = (me * local).astype(F32)

    def reset_base():
        base_r[...] = jnp.zeros_like(base_r)
        base_c[...] = jnp.zeros_like(base_c)

    def pack_slot(j, carry):
        ids = meta[j, 0:top_k, :]
        gts = meta[j, top_k:2 * top_k, :]
        rel = ids - lo
        chosen = jnp.max(jnp.where((rel >= 0) & (rel < local), 1.0, 0.0), axis=0, keepdims=True)
        halves = []
        for c in range(2):
            ch = jnp.broadcast_to(chosen[:, c * tok_dev:(c + 1) * tok_dev], (8, tok_dev)).astype(BF16)
            halves.append(dot(ch, tri[...])[0:1, :] + float(c * cap))
        rank2 = jnp.where(chosen > 0, jnp.concatenate(halves, axis=1), -1.0)
        pack = jnp.where(rank2 == lax.broadcasted_iota(jnp.int32, (blk, 2 * tok_dev), 0).astype(F32), 1.0, 0.0)
        pack_b = pack.astype(BF16)
        loc_iota = lax.broadcasted_iota(jnp.int32, (local, 2 * tok_dev), 0).astype(F32)
        mem = jnp.zeros((local, 2 * tok_dev), F32)
        gat = jnp.zeros((local, 2 * tok_dev), F32)
        for i in range(top_k):
            hit = rel[i:i + 1, :] == loc_iota
            mem = jnp.where(hit, 1.0, mem)
            gat = jnp.where(hit, gts[i:i + 1, :], gat)
        mem_b = mem.astype(BF16)
        mem_r = dot_nt(mem_b, pack_b)
        mem_c = dot_nt(pack_b, mem_b)
        gate_j = dot_nt(pack, gat, lax.Precision.HIGHEST)
        tri_b = tri[0:blk, 0:blk]
        pos_r = dot(mem_r.astype(BF16), tri_b) + base_r[...]
        pos_c = dot_tn(tri_b, mem_c.astype(BF16)) + base_c[...]
        here = pl.ds(pl.multiple_of(j * blk, blk), blk)
        slot_r[:, here] = jnp.where(mem_r > 0, pos_r, -1.0)
        slot_c[here, :] = jnp.where(mem_c > 0, pos_c, -1.0)
        gate_c[here, :] = gate_j
        base_r[...] += jnp.sum(mem_r, axis=1, keepdims=True)
        base_c[...] += jnp.sum(mem_c, axis=0, keepdims=True)

        def tile(n, carry):
            cols = pl.ds(pl.multiple_of(n * nt, nt), nt)
            rows[here, cols] = dot(pack_b, xall[j, :, cols]).astype(BF16)
            return carry

        lax.fori_loop(0, d_model // nt, tile, 0)
        return carry

    def expert_pass(j0, j1, last, hook):
        r0, count = j0 * blk, (j1 - j0) * blk

        def zero(i, carry):
            acc[pl.ds(pl.multiple_of(i * blk, blk), blk), :] = jnp.zeros((blk, d_model), F32)
            return carry

        lax.fori_loop(0, j1 - j0, zero, 0)

        def expert(l, carry):
            slot = l % 2
            hook(l)

            def prefetch():
                for copy in weight_copies((l + 1) % local, (l + 1) % 2):
                    copy.start()

            if last:
                pl.when(l < local - 1)(prefetch)
            else:
                prefetch()
            lane = lax.broadcasted_iota(jnp.int32, (count, local), 1) == l
            pos = jnp.sum(jnp.where(lane, slot_c[r0:r0 + count, :], 0.0), axis=1, keepdims=True)
            gate = jnp.sum(jnp.where(lane, gate_c[r0:r0 + count, :], 0.0), axis=1, keepdims=True)
            fan_t[0:count, :] = jnp.where(pos == lax.broadcasted_iota(jnp.int32, (count, ecap), 1).astype(F32), 1.0, 0.0).astype(BF16)
            row_pos = slot_r[pl.ds(l, 1), r0:r0 + count]
            fan[:, 0:count] = jnp.where(row_pos == lax.broadcasted_iota(jnp.int32, (ecap, count), 0).astype(F32), 1.0, 0.0).astype(BF16)

            def gather(n, carry):
                cols = pl.ds(pl.multiple_of(n * nt, nt), nt)
                xin[:, cols] = dot(fan[:, 0:count], rows[r0:r0 + count, cols]).astype(BF16)
                return carry

            lax.fori_loop(0, d_model // nt, gather, 0)
            copies = weight_copies(l, slot)
            copies[0].wait()
            copies[1].wait()

            def inner(f, carry):
                cols = pl.ds(pl.multiple_of(f * ft, ft), ft)
                gate_act = dot(xin[...], wgb[slot, :, cols])
                up_act = dot(xin[...], wub[slot, :, cols])
                hid[:, cols] = (jax.nn.silu(gate_act) * up_act).astype(BF16)
                return carry

            lax.fori_loop(0, ffn // ft, inner, 0)
            copies[2].wait()

            def down(n, carry):
                cols = pl.ds(pl.multiple_of(n * nt, nt), nt)
                y = dot(hid[...], wdb[slot, :, cols]).astype(BF16)
                acc[0:count, cols] += gate * dot(fan_t[0:count, :], y)
                return carry

            lax.fori_loop(0, d_model // nt, down, 0)
            return carry

        lax.fori_loop(0, local, expert, 0)

        def finish(i, carry):
            rows[pl.ds(pl.multiple_of(r0 + i * blk, blk), blk), :] = acc[pl.ds(pl.multiple_of(i * blk, blk), blk), :].astype(BF16)
            return carry

        lax.fori_loop(0, j1 - j0, finish, 0)

    reset_base()
    own_tok.wait()
    wait_sib(0)
    lax.fori_loop(0, 1, pack_slot, 0)
    for s in range(1, half - 1):
        jr, jl = 2 * s - 1, 2 * s
        relay_meta(jr, jr + 2, right)
        relay_meta(jl, jl + 2, left)
        for sub in range(SUBS):
            relay_sub(jr, sub, jr + 2, right)
            relay_sub(jl, sub, jl + 2, left)
        wait_sib(jr)
        wait_sib(jl)
        lax.fori_loop(jr, jl + 1, pack_slot, 0)

    jr, jl = split, split + 1

    def hook_a(l):
        def meta_step():
            relay_meta(jr, far, right)
            relay_meta(jl, None, left)

        def data_step():
            sub = l - 2
            for j, dev, toward in ((jr, right, sub < SUBS // 2), (jl, left, sub >= SUBS // 2)):
                here = xall.at[j, sub_ds(sub)]
                ring_copy(here, j, sub, dev).wait_recv()

                def forward():
                    ring_copy(here, far, sub, dev).start()

                pl.when(toward)(forward)
                sib_copy(here, j, sub).start()

        pl.when(l == 1)(meta_step)
        pl.when((l >= 2) & (l < 2 + SUBS))(data_step)

    expert_pass(0, split, False, hook_a)
    ret[0:cap, :] = rows[0:cap, :]
    for j in list(range(split - 1, -1, -1)):
        for c in range(2):
            if (j, c) != (0, 0):
                ret_copy(j, c).start()

    relay_meta(far, None, right)
    for sub in range(SUBS):
        relay_sub(far, sub, None, right)
    reset_base()
    for j in (jr, jl, far):
        wait_sib(j)
    lax.fori_loop(split, nz, pack_slot, 0)
    expert_pass(split, nz, True, lambda l: None)
    for j in range(nz - 1, split - 1, -1):
        for c in range(2):
            ret_copy(j, c).start()

    near = split * blk
    for j in range(split):
        for c in range(2):
            if (j, c) != (0, 0):
                ret_copy(j, c).wait_recv()

    def first(n, carry):
        cols = pl.ds(pl.multiple_of(n * nt, nt), nt)
        acc[0:tok_dev, cols] = xall[0, 0:tok_dev, cols].astype(F32) + dot_tn(comb[0:near, :], ret[0:near, cols])
        return carry

    lax.fori_loop(0, d_model // nt, first, 0)
    for j in range(split, nz):
        for c in range(2):
            ret_copy(j, c).wait_recv()

    def second(n, carry):
        cols = pl.ds(pl.multiple_of(n * nt, nt), nt)
        out[:, cols] = (acc[0:tok_dev, cols] + dot_tn(comb[near:, :], ret[near:, cols])).astype(BF16)
        return carry

    lax.fori_loop(0, d_model // nt, second, 0)

    for j in range(nz):
        msib_copy(meta_in, j).wait_send()
        if j > 0:
            mring_copy(meta_in, j, right).wait_send()
        for sub in range(SUBS):
            sib_copy(tok.at[sub_ds(sub)], j, sub).wait_send()
            if j > 0:
                ring_copy(tok.at[sub_ds(sub)], j, sub, right).wait_send()
        for c in range(2):
            if (j, c) != (0, 0):
                ret_copy(j, c).wait_send()


def solution(mesh):
    groups = mesh.shape['ep']
    nz = groups // 2
    row_spec = P(('dp', 'ep'))
    expert_spec = P('ep')

    def device_step(tokens, expert_ids, gate_vals, w_gate, w_up, w_down):
        tok_dev, top_k = expert_ids.shape
        d_model = tokens.shape[1]
        local, _, ffn = w_gate.shape
        cap = tok_dev * (top_k // 2) // groups
        ecap = tok_dev * top_k // local
        row_count = groups * cap
        near = (2 * (nz // 2) - 3) * 2 * cap
        meta = jnp.concatenate([expert_ids.T.astype(F32), gate_vals.T], axis=0)
        hbm = pl.BlockSpec(memory_space=pl.ANY)
        dma = pltpu.SemaphoreType.DMA
        return pl.pallas_call(
            functools.partial(moe_kernel, groups),
            out_shape=jax.ShapeDtypeStruct(tokens.shape, tokens.dtype),
            in_specs=[hbm] * 5,
            out_specs=pl.BlockSpec(memory_space=pltpu.VMEM),
            scratch_shapes=[
                pltpu.VMEM((nz, 2 * tok_dev, d_model), BF16),
                pltpu.VMEM((nz, 2 * top_k, 2 * tok_dev), F32),
                pltpu.VMEM((row_count, d_model), BF16),
                pltpu.VMEM((near, d_model), F32),
                pltpu.VMEM((row_count, d_model), BF16),
                pltpu.VMEM((2, d_model, ffn), BF16),
                pltpu.VMEM((2, d_model, ffn), BF16),
                pltpu.VMEM((2, ffn, d_model), BF16),
                pltpu.VMEM((ecap, d_model), BF16),
                pltpu.VMEM((ecap, ffn), BF16),
                pltpu.VMEM((ecap, near), BF16),
                pltpu.VMEM((near, ecap), BF16),
                pltpu.VMEM((local, row_count), F32),
                pltpu.VMEM((row_count, local), F32),
                pltpu.VMEM((row_count, local), F32),
                pltpu.VMEM((row_count, tok_dev), BF16),
                pltpu.VMEM((tok_dev, tok_dev), BF16),
                pltpu.VMEM((local, 1), F32),
                pltpu.VMEM((1, local), F32),
                dma((nz, SUBS)), dma((nz, SUBS)), dma((nz, SUBS)), dma((nz, SUBS)),
                dma((nz,)), dma((nz,)), dma((nz,)), dma((nz,)),
                dma((nz, 2)), dma((nz, 2)), dma((2, 3)), dma((2,)),
            ],
            compiler_params=pltpu.CompilerParams(collective_id=0, has_side_effects=True, vmem_limit_bytes=67043328),
            name='moe_fused',
        )(tokens, meta, w_gate, w_up, w_down)

    return jax.shard_map(device_step, mesh=mesh, in_specs=(row_spec, row_spec, row_spec, expert_spec, expert_spec, expert_spec), out_specs=row_spec, check_vma=False)
```

```python
import functools

import jax
import jax.numpy as jnp
from jax import lax
from jax.experimental import pallas as pl
from jax.experimental.pallas import tpu as pltpu
from jax.sharding import PartitionSpec as P

MESH = pl.DeviceIdType.MESH
SUBS = 4
F32 = jnp.float32
BF16 = jnp.bfloat16


def dot(a, b):
    return jnp.dot(a, b, preferred_element_type=F32)


def dot_nt(a, b, precision=None):
    return lax.dot_general(a, b, (((1,), (1,)), ((), ())), precision=precision, preferred_element_type=F32)


def dot_tn(a, b):
    return lax.dot_general(a, b, (((0,), (0,)), ((), ())), preferred_element_type=F32)


def moe_kernel(groups, tok, meta_in, w_gate, w_up, w_down, out, xall, meta, rows, acc, ret, wgb, wub, wdb, xin, hid, fan, fan_t,
               slot_r, slot_c, gate_c, comb, tri, base_r, base_c, ring_s, ring_r, sib_s, sib_r, mring_s, mring_r, msib_s, msib_r,
               ret_s, ret_r, wsem, loc):
    nz = groups // 2
    half = nz // 2
    tok_dev, d_model = tok.shape
    local, _, ffn = w_gate.shape
    top_k = meta.shape[1] // 2
    cap = tok_dev * (top_k // 2) // groups
    ecap = fan.shape[0]
    sub_rows = tok_dev // SUBS
    blk = 2 * cap
    nt = min(512, d_model)
    ft = min(256, ffn)
    far = nz - 1
    split = 2 * half - 3

    me = lax.axis_index('ep')
    z = me // 2
    k = me % 2
    right = ((z + 1) % nz) * 2 + k
    left = ((z + nz - 1) % nz) * 2 + k
    sib = z * 2 + 1 - k

    def source_shift(j):
        if j == 0:
            return 0
        if j == far:
            return half
        return nz - (j + 1) // 2 if j % 2 == 1 else j // 2

    def device_at(shift, c):
        return ((z + shift) % nz) * 2 + (k if c == 0 else 1 - k)

    def remote(src, dst, ssem, rsem, dev):
        return pltpu.make_async_remote_copy(src_ref=src, dst_ref=dst, send_sem=ssem, recv_sem=rsem, device_id={'ep': dev}, device_id_type=MESH)

    def sub_ds(sub, c=0):
        return pl.ds(c * tok_dev + sub * sub_rows, sub_rows)

    def ring_copy(src, dst_j, sub, dev):
        return remote(src, xall.at[dst_j, sub_ds(sub)], ring_s.at[dst_j, sub], ring_r.at[dst_j, sub], dev)

    def sib_copy(src, j, sub):
        return remote(src, xall.at[j, sub_ds(sub, 1)], sib_s.at[j, sub], sib_r.at[j, sub], sib)

    def mring_copy(src, dst_j, dev):
        return remote(src, meta.at[dst_j, :, pl.ds(0, tok_dev)], mring_s.at[dst_j], mring_r.at[dst_j], dev)

    def msib_copy(src, j):
        return remote(src, meta.at[j, :, pl.ds(tok_dev, tok_dev)], msib_s.at[j], msib_r.at[j], sib)

    def ret_copy(j, c):
        off = j * blk + c * cap
        return remote(rows.at[pl.ds(off, cap)], ret.at[pl.ds(off, cap)], ret_s.at[j, c], ret_r.at[j, c], device_at(source_shift(j), c))

    def weight_copies(expert, slot):
        return (pltpu.make_async_copy(w_gate.at[expert], wgb.at[slot], wsem.at[slot, 0]),
                pltpu.make_async_copy(w_up.at[expert], wub.at[slot], wsem.at[slot, 1]),
                pltpu.make_async_copy(w_down.at[expert], wdb.at[slot], wsem.at[slot, 2]))

    own_tok = pltpu.make_async_copy(tok, xall.at[0, pl.ds(0, tok_dev)], loc.at[0])
    own_meta = pltpu.make_async_copy(meta_in, meta.at[0, :, pl.ds(0, tok_dev)], loc.at[1])
    own_meta.start()
    own_tok.start()

    barrier = pltpu.get_barrier_semaphore()
    for step in range(1, groups):
        pl.semaphore_signal(barrier, inc=1, device_id={'ep': (me + step) % groups}, device_id_type=MESH)
    pl.semaphore_wait(barrier, groups - 1)

    mring_copy(meta_in, 1, right).start()
    mring_copy(meta_in, 2, left).start()
    msib_copy(meta_in, 0).start()
    for sub in range(SUBS):
        ring_copy(tok.at[sub_ds(sub)], 1, sub, right).start()
        ring_copy(tok.at[sub_ds(sub)], 2, sub, left).start()
    for sub in range(SUBS):
        sib_copy(tok.at[sub_ds(sub)], 0, sub).start()
    for copy in weight_copies(0, 0):
        copy.start()

    def relay_meta(j, next_j, dev):
        mring_copy(meta_in, j, dev).wait_recv()
        here = meta.at[j, :, pl.ds(0, tok_dev)]
        if next_j is not None:
            mring_copy(here, next_j, dev).start()
        msib_copy(here, j).start()

    def relay_sub(j, sub, next_j, dev):
        here = xall.at[j, sub_ds(sub)]
        ring_copy(here, j, sub, dev).wait_recv()
        if next_j is not None:
            ring_copy(here, next_j, sub, dev).start()
        sib_copy(here, j, sub).start()

    def wait_sib(j):
        msib_copy(meta.at[j, :, pl.ds(0, tok_dev)], j).wait_recv()
        for sub in range(SUBS):
            sib_copy(xall.at[j, sub_ds(sub)], j, sub).wait_recv()

    tok_row = lax.broadcasted_iota(jnp.int32, (tok_dev, tok_dev), 0)
    tok_col = lax.broadcasted_iota(jnp.int32, (tok_dev, tok_dev), 1)
    tri[...] = jnp.where(tok_row < tok_col, 1.0, 0.0).astype(BF16)

    own_meta.wait()
    row_id = lax.broadcasted_iota(jnp.int32, (2 * nz, tok_dev), 0)
    peer_lo = jnp.zeros((2 * nz, tok_dev), jnp.int32)
    for j in range(nz):
        for c in range(2):
            peer = device_at((nz - source_shift(j)) % nz, c)
            peer_lo = jnp.where(row_id == 2 * j + c, peer * local, peer_lo)
    peer_lo = peer_lo.astype(F32)
    own_ids = meta[0, 0:top_k, 0:tok_dev]
    picked = jnp.zeros((2 * nz, tok_dev), F32)
    for i in range(top_k):
        rel = own_ids[i:i + 1, :] - peer_lo
        picked = jnp.where((rel >= 0) & (rel < local), 1.0, picked)
    rank = jnp.where(picked > 0, dot(picked.astype(BF16), tri[...]), -1.0)
    cap_iota = lax.broadcasted_iota(jnp.int32, (cap, tok_dev), 0).astype(F32)
    for r in range(2 * nz):
        comb[r * cap:(r + 1) * cap, :] = jnp.where(rank[r:r + 1, :] == cap_iota, 1.0, 0.0).astype(BF16)

    lo = (me * local).astype(F32)

    def reset_base():
        base_r[...] = jnp.zeros_like(base_r)
        base_c[...] = jnp.zeros_like(base_c)

    def pack_slot(j, carry):
        ids = meta[j, 0:top_k, :]
        gts = meta[j, top_k:2 * top_k, :]
        rel = ids - lo
        chosen = jnp.max(jnp.where((rel >= 0) & (rel < local), 1.0, 0.0), axis=0, keepdims=True)
        halves = []
        for c in range(2):
            ch = jnp.broadcast_to(chosen[:, c * tok_dev:(c + 1) * tok_dev], (8, tok_dev)).astype(BF16)
            halves.append(dot(ch, tri[...])[0:1, :] + float(c * cap))
        rank2 = jnp.where(chosen > 0, jnp.concatenate(halves, axis=1), -1.0)
        pack = jnp.where(rank2 == lax.broadcasted_iota(jnp.int32, (blk, 2 * tok_dev), 0).astype(F32), 1.0, 0.0)
        pack_b = pack.astype(BF16)
        loc_iota = lax.broadcasted_iota(jnp.int32, (local, 2 * tok_dev), 0).astype(F32)
        mem = jnp.zeros((local, 2 * tok_dev), F32)
        gat = jnp.zeros((local, 2 * tok_dev), F32)
        for i in range(top_k):
            hit = rel[i:i + 1, :] == loc_iota
            mem = jnp.where(hit, 1.0, mem)
            gat = jnp.where(hit, gts[i:i + 1, :], gat)
        mem_b = mem.astype(BF16)
        mem_r = dot_nt(mem_b, pack_b)
        mem_c = dot_nt(pack_b, mem_b)
        gate_j = dot_nt(pack, gat, lax.Precision.HIGHEST)
        tri_b = tri[0:blk, 0:blk]
        pos_r = dot(mem_r.astype(BF16), tri_b) + base_r[...]
        pos_c = dot_tn(tri_b, mem_c.astype(BF16)) + base_c[...]
        here = pl.ds(pl.multiple_of(j * blk, blk), blk)
        slot_r[:, here] = jnp.where(mem_r > 0, pos_r, -1.0)
        slot_c[here, :] = jnp.where(mem_c > 0, pos_c, -1.0)
        gate_c[here, :] = gate_j
        base_r[...] += jnp.sum(mem_r, axis=1, keepdims=True)
        base_c[...] += jnp.sum(mem_c, axis=0, keepdims=True)

        def tile(n, carry):
            cols = pl.ds(pl.multiple_of(n * nt, nt), nt)
            rows[here, cols] = dot(pack_b, xall[j, :, cols]).astype(BF16)
            return carry

        lax.fori_loop(0, d_model // nt, tile, 0)
        return carry

    def expert_pass(j0, j1, last, hook):
        r0, count = j0 * blk, (j1 - j0) * blk

        def zero(i, carry):
            acc[pl.ds(pl.multiple_of(i * blk, blk), blk), :] = jnp.zeros((blk, d_model), F32)
            return carry

        lax.fori_loop(0, j1 - j0, zero, 0)

        def expert(l, carry):
            slot = l % 2
            hook(l)

            def prefetch():
                for copy in weight_copies((l + 1) % local, (l + 1) % 2):
                    copy.start()

            if last:
                pl.when(l < local - 1)(prefetch)
            else:
                prefetch()
            lane = lax.broadcasted_iota(jnp.int32, (count, local), 1) == l
            pos = jnp.sum(jnp.where(lane, slot_c[r0:r0 + count, :], 0.0), axis=1, keepdims=True)
            gate = jnp.sum(jnp.where(lane, gate_c[r0:r0 + count, :], 0.0), axis=1, keepdims=True)
            fan_t[0:count, :] = jnp.where(pos == lax.broadcasted_iota(jnp.int32, (count, ecap), 1).astype(F32), 1.0, 0.0).astype(BF16)
            row_pos = slot_r[pl.ds(l, 1), r0:r0 + count]
            fan[:, 0:count] = jnp.where(row_pos == lax.broadcasted_iota(jnp.int32, (ecap, count), 0).astype(F32), 1.0, 0.0).astype(BF16)

            for copy in weight_copies(l, slot):
                copy.wait()
            for n in range(0, d_model, nt):
                xin[:, n:n + nt] = dot(fan[:, 0:count], rows[r0:r0 + count, n:n + nt]).astype(BF16)
            for f in range(0, ffn, ft):
                gate_act = dot(xin[...], wgb[slot, :, f:f + ft])
                up_act = dot(xin[...], wub[slot, :, f:f + ft])
                hid[:, f:f + ft] = (jax.nn.silu(gate_act) * up_act).astype(BF16)
            for n in range(0, d_model, nt):
                y = dot(hid[...], wdb[slot, :, n:n + nt]).astype(BF16)
                acc[0:count, n:n + nt] += gate * dot(fan_t[0:count, :], y)
            return carry

        lax.fori_loop(0, local, expert, 0)

        def finish(i, carry):
            rows[pl.ds(pl.multiple_of(r0 + i * blk, blk), blk), :] = acc[pl.ds(pl.multiple_of(i * blk, blk), blk), :].astype(BF16)
            return carry

        lax.fori_loop(0, j1 - j0, finish, 0)

    reset_base()
    own_tok.wait()
    wait_sib(0)
    lax.fori_loop(0, 1, pack_slot, 0)
    for s in range(1, half - 1):
        jr, jl = 2 * s - 1, 2 * s
        relay_meta(jr, jr + 2, right)
        relay_meta(jl, jl + 2, left)
        for sub in range(SUBS):
            relay_sub(jr, sub, jr + 2, right)
            relay_sub(jl, sub, jl + 2, left)
        wait_sib(jr)
        wait_sib(jl)
        lax.fori_loop(jr, jl + 1, pack_slot, 0)

    jr, jl = split, split + 1

    def hook_a(l):
        def meta_step():
            relay_meta(jr, far, right)
            relay_meta(jl, None, left)

        def data_step():
            sub = l - 2
            for j, dev, toward in ((jr, right, sub < SUBS // 2), (jl, left, sub >= SUBS // 2)):
                here = xall.at[j, sub_ds(sub)]
                ring_copy(here, j, sub, dev).wait_recv()

                def forward():
                    ring_copy(here, far, sub, dev).start()

                pl.when(toward)(forward)
                sib_copy(here, j, sub).start()

        pl.when(l == 1)(meta_step)
        pl.when((l >= 2) & (l < 2 + SUBS))(data_step)

    expert_pass(0, split, False, hook_a)
    ret[0:cap, :] = rows[0:cap, :]
    for j in list(range(split - 1, -1, -1)):
        for c in range(2):
            if (j, c) != (0, 0):
                ret_copy(j, c).start()

    relay_meta(far, None, right)
    for sub in range(SUBS):
        relay_sub(far, sub, None, right)
    reset_base()
    for j in (jr, jl, far):
        wait_sib(j)
    lax.fori_loop(split, nz, pack_slot, 0)
    expert_pass(split, nz, True, lambda l: None)
    for j in range(nz - 1, split - 1, -1):
        for c in range(2):
            ret_copy(j, c).start()

    near = split * blk
    for j in range(split):
        for c in range(2):
            if (j, c) != (0, 0):
                ret_copy(j, c).wait_recv()

    def first(n, carry):
        cols = pl.ds(pl.multiple_of(n * nt, nt), nt)
        acc[0:tok_dev, cols] = xall[0, 0:tok_dev, cols].astype(F32) + dot_tn(comb[0:near, :], ret[0:near, cols])
        return carry

    lax.fori_loop(0, d_model // nt, first, 0)
    for j in range(split, nz):
        for c in range(2):
            ret_copy(j, c).wait_recv()

    def second(n, carry):
        cols = pl.ds(pl.multiple_of(n * nt, nt), nt)
        out[:, cols] = (acc[0:tok_dev, cols] + dot_tn(comb[near:, :], ret[near:, cols])).astype(BF16)
        return carry

    lax.fori_loop(0, d_model // nt, second, 0)

    for j in range(nz):
        msib_copy(meta_in, j).wait_send()
        if j > 0:
            mring_copy(meta_in, j, right).wait_send()
        for sub in range(SUBS):
            sib_copy(tok.at[sub_ds(sub)], j, sub).wait_send()
            if j > 0:
                ring_copy(tok.at[sub_ds(sub)], j, sub, right).wait_send()
        for c in range(2):
            if (j, c) != (0, 0):
                ret_copy(j, c).wait_send()


def solution(mesh):
    groups = mesh.shape['ep']
    nz = groups // 2
    row_spec = P(('dp', 'ep'))
    expert_spec = P('ep')

    def device_step(tokens, expert_ids, gate_vals, w_gate, w_up, w_down):
        tok_dev, top_k = expert_ids.shape
        d_model = tokens.shape[1]
        local, _, ffn = w_gate.shape
        cap = tok_dev * (top_k // 2) // groups
        ecap = tok_dev * top_k // local
        row_count = groups * cap
        near = (2 * (nz // 2) - 3) * 2 * cap
        meta = jnp.concatenate([expert_ids.T.astype(F32), gate_vals.T], axis=0)
        hbm = pl.BlockSpec(memory_space=pl.ANY)
        dma = pltpu.SemaphoreType.DMA
        return pl.pallas_call(
            functools.partial(moe_kernel, groups),
            out_shape=jax.ShapeDtypeStruct(tokens.shape, tokens.dtype),
            in_specs=[hbm] * 5,
            out_specs=pl.BlockSpec(memory_space=pltpu.VMEM),
            scratch_shapes=[
                pltpu.VMEM((nz, 2 * tok_dev, d_model), BF16),
                pltpu.VMEM((nz, 2 * top_k, 2 * tok_dev), F32),
                pltpu.VMEM((row_count, d_model), BF16),
                pltpu.VMEM((near, d_model), F32),
                pltpu.VMEM((row_count, d_model), BF16),
                pltpu.VMEM((2, d_model, ffn), BF16),
                pltpu.VMEM((2, d_model, ffn), BF16),
                pltpu.VMEM((2, ffn, d_model), BF16),
                pltpu.VMEM((ecap, d_model), BF16),
                pltpu.VMEM((ecap, ffn), BF16),
                pltpu.VMEM((ecap, near), BF16),
                pltpu.VMEM((near, ecap), BF16),
                pltpu.VMEM((local, row_count), F32),
                pltpu.VMEM((row_count, local), F32),
                pltpu.VMEM((row_count, local), F32),
                pltpu.VMEM((row_count, tok_dev), BF16),
                pltpu.VMEM((tok_dev, tok_dev), BF16),
                pltpu.VMEM((local, 1), F32),
                pltpu.VMEM((1, local), F32),
                dma((nz, SUBS)), dma((nz, SUBS)), dma((nz, SUBS)), dma((nz, SUBS)),
                dma((nz,)), dma((nz,)), dma((nz,)), dma((nz,)),
                dma((nz, 2)), dma((nz, 2)), dma((2, 3)), dma((2,)),
            ],
            compiler_params=pltpu.CompilerParams(collective_id=0, has_side_effects=True, vmem_limit_bytes=67043328),
            name='moe_fused',
        )(tokens, meta, w_gate, w_up, w_down)

    return jax.shard_map(device_step, mesh=mesh, in_specs=(row_spec, row_spec, row_spec, expert_spec, expert_spec, expert_spec), out_specs=row_spec, check_vma=False)
```

```python
import functools

import jax
import jax.numpy as jnp
from jax import lax
from jax.experimental import pallas as pl
from jax.experimental.pallas import tpu as pltpu
from jax.sharding import PartitionSpec as P

MESH = pl.DeviceIdType.MESH
SUBS = 4
F32 = jnp.float32
BF16 = jnp.bfloat16


def dot(a, b):
    return jnp.dot(a, b, preferred_element_type=F32)


def dot_nt(a, b, precision=None):
    return lax.dot_general(a, b, (((1,), (1,)), ((), ())), precision=precision, preferred_element_type=F32)


def dot_tn(a, b):
    return lax.dot_general(a, b, (((0,), (0,)), ((), ())), preferred_element_type=F32)


def moe_kernel(groups, tok, ids_in, gates_in, w_gate, w_up, w_down, out, xall, ids_all, gates_all, rows, acc, ret, wgb, wub, wdb, xin, hid, fan, fan_t,
               slot_r, slot_c, gate_c, comb, tri, base_r, base_c, ring_s, ring_r, sib_s, sib_r, mring_s, mring_r, msib_s, msib_r,
               ret_s, ret_r, wsem, loc):
    nz = groups // 2
    half = nz // 2
    tok_dev, d_model = tok.shape
    local, _, ffn = w_gate.shape
    top_k = ids_in.shape[0]
    cap = tok_dev * (top_k // 2) // groups
    ecap = fan.shape[0]
    sub_rows = tok_dev // SUBS
    blk = 2 * cap
    nt = min(512, d_model)
    ft = min(256, ffn)
    far = nz - 1
    split = 2 * half - 3

    me = lax.axis_index('ep')
    z = me // 2
    k = me % 2
    right = ((z + 1) % nz) * 2 + k
    left = ((z + nz - 1) % nz) * 2 + k
    sib = z * 2 + 1 - k

    def source_shift(j):
        if j == 0:
            return 0
        if j == far:
            return half
        return nz - (j + 1) // 2 if j % 2 == 1 else j // 2

    def device_at(shift, c):
        return ((z + shift) % nz) * 2 + (k if c == 0 else 1 - k)

    def remote(src, dst, ssem, rsem, dev):
        return pltpu.make_async_remote_copy(src_ref=src, dst_ref=dst, send_sem=ssem, recv_sem=rsem, device_id={'ep': dev}, device_id_type=MESH)

    def sub_ds(sub, c=0):
        return pl.ds(c * tok_dev + sub * sub_rows, sub_rows)

    def ring_copy(src, dst_j, sub, dev):
        return remote(src, xall.at[dst_j, sub_ds(sub)], ring_s.at[dst_j, sub], ring_r.at[dst_j, sub], dev)

    def sib_copy(src, j, sub):
        return remote(src, xall.at[j, sub_ds(sub, 1)], sib_s.at[j, sub], sib_r.at[j, sub], sib)

    tables = ((ids_in, ids_all), (gates_in, gates_all))

    def table_src(i, j, own):
        return tables[i][0] if own else tables[i][1].at[j, :, pl.ds(0, tok_dev)]

    def mring_copy(i, src_j, dst_j, dev):
        return remote(table_src(i, src_j, src_j == 0), tables[i][1].at[dst_j, :, pl.ds(0, tok_dev)], mring_s.at[dst_j, i], mring_r.at[dst_j, i], dev)

    def msib_copy(i, j):
        return remote(table_src(i, j, j == 0), tables[i][1].at[j, :, pl.ds(tok_dev, tok_dev)], msib_s.at[j, i], msib_r.at[j, i], sib)

    def ret_copy(j, c):
        off = j * blk + c * cap
        return remote(rows.at[pl.ds(off, cap)], ret.at[pl.ds(off, cap)], ret_s.at[j, c], ret_r.at[j, c], device_at(source_shift(j), c))

    def weight_copies(expert, slot):
        return (pltpu.make_async_copy(w_gate.at[expert], wgb.at[slot], wsem.at[slot, 0]),
                pltpu.make_async_copy(w_up.at[expert], wub.at[slot], wsem.at[slot, 1]),
                pltpu.make_async_copy(w_down.at[expert], wdb.at[slot], wsem.at[slot, 2]))

    own_tok = pltpu.make_async_copy(tok, xall.at[0, pl.ds(0, tok_dev)], loc.at[0])
    own_tables = [pltpu.make_async_copy(tables[i][0], tables[i][1].at[0, :, pl.ds(0, tok_dev)], loc.at[1 + i]) for i in range(2)]
    for copy in own_tables:
        copy.start()
    own_tok.start()

    barrier = pltpu.get_barrier_semaphore()
    for step in range(1, groups):
        pl.semaphore_signal(barrier, inc=1, device_id={'ep': (me + step) % groups}, device_id_type=MESH)
    pl.semaphore_wait(barrier, groups - 1)

    for i in range(2):
        mring_copy(i, 0, 1, right).start()
        mring_copy(i, 0, 2, left).start()
        msib_copy(i, 0).start()
    for sub in range(SUBS):
        ring_copy(tok.at[sub_ds(sub)], 1, sub, right).start()
        ring_copy(tok.at[sub_ds(sub)], 2, sub, left).start()
    for sub in range(SUBS):
        sib_copy(tok.at[sub_ds(sub)], 0, sub).start()
    for copy in weight_copies(0, 0):
        copy.start()

    def relay_meta(j, next_j, dev):
        for i in range(2):
            mring_copy(i, j, j, dev).wait_recv()
            if next_j is not None:
                mring_copy(i, j, next_j, dev).start()
            msib_copy(i, j).start()

    def relay_sub(j, sub, next_j, dev):
        here = xall.at[j, sub_ds(sub)]
        ring_copy(here, j, sub, dev).wait_recv()
        if next_j is not None:
            ring_copy(here, next_j, sub, dev).start()
        sib_copy(here, j, sub).start()

    def wait_sib(j):
        for i in range(2):
            msib_copy(i, j).wait_recv()
        for sub in range(SUBS):
            sib_copy(xall.at[j, sub_ds(sub)], j, sub).wait_recv()

    tok_row = lax.broadcasted_iota(jnp.int32, (tok_dev, tok_dev), 0)
    tok_col = lax.broadcasted_iota(jnp.int32, (tok_dev, tok_dev), 1)
    tri[...] = jnp.where(tok_row < tok_col, 1.0, 0.0).astype(BF16)

    for copy in own_tables:
        copy.wait()
    row_id = lax.broadcasted_iota(jnp.int32, (2 * nz, tok_dev), 0)
    peer_lo = jnp.zeros((2 * nz, tok_dev), jnp.int32)
    for j in range(nz):
        for c in range(2):
            peer = device_at((nz - source_shift(j)) % nz, c)
            peer_lo = jnp.where(row_id == 2 * j + c, peer * local, peer_lo)
    own_ids = ids_all[0, :, 0:tok_dev]
    picked = jnp.zeros((2 * nz, tok_dev), F32)
    for i in range(top_k):
        rel = own_ids[i:i + 1, :] - peer_lo
        picked = jnp.where((rel >= 0) & (rel < local), 1.0, picked)
    rank = jnp.where(picked > 0, dot(picked.astype(BF16), tri[...]), -1.0)
    cap_iota = lax.broadcasted_iota(jnp.int32, (cap, tok_dev), 0).astype(F32)
    for r in range(2 * nz):
        comb[r * cap:(r + 1) * cap, :] = jnp.where(rank[r:r + 1, :] == cap_iota, 1.0, 0.0).astype(BF16)

    lo = me * local

    def reset_base():
        base_r[...] = jnp.zeros_like(base_r)
        base_c[...] = jnp.zeros_like(base_c)

    def pack_slot(j, carry):
        gts = gates_all[j]
        rel = ids_all[j] - lo
        chosen = jnp.max(jnp.where((rel >= 0) & (rel < local), 1.0, 0.0), axis=0, keepdims=True)
        halves = []
        for c in range(2):
            ch = jnp.broadcast_to(chosen[:, c * tok_dev:(c + 1) * tok_dev], (8, tok_dev)).astype(BF16)
            halves.append(dot(ch, tri[...])[0:1, :] + float(c * cap))
        rank2 = jnp.where(chosen > 0, jnp.concatenate(halves, axis=1), -1.0)
        pack = jnp.where(rank2 == lax.broadcasted_iota(jnp.int32, (blk, 2 * tok_dev), 0).astype(F32), 1.0, 0.0)
        pack_b = pack.astype(BF16)
        loc_iota = lax.broadcasted_iota(jnp.int32, (local, 2 * tok_dev), 0)
        mem = jnp.zeros((local, 2 * tok_dev), F32)
        gat = jnp.zeros((local, 2 * tok_dev), F32)
        for i in range(top_k):
            hit = rel[i:i + 1, :] == loc_iota
            mem = jnp.where(hit, 1.0, mem)
            gat = jnp.where(hit, gts[i:i + 1, :], gat)
        mem_b = mem.astype(BF16)
        mem_r = dot_nt(mem_b, pack_b)
        mem_c = dot_nt(pack_b, mem_b)
        gate_j = dot_nt(pack, gat, lax.Precision.HIGHEST)
        tri_b = tri[0:blk, 0:blk]
        pos_r = dot(mem_r.astype(BF16), tri_b) + base_r[...]
        pos_c = dot_tn(tri_b, mem_c.astype(BF16)) + base_c[...]
        here = pl.ds(pl.multiple_of(j * blk, blk), blk)
        slot_r[:, here] = jnp.where(mem_r > 0, pos_r, -1.0)
        slot_c[here, :] = jnp.where(mem_c > 0, pos_c, -1.0)
        gate_c[here, :] = gate_j
        base_r[...] += jnp.sum(mem_r, axis=1, keepdims=True)
        base_c[...] += jnp.sum(mem_c, axis=0, keepdims=True)

        for n in range(0, d_model, nt):
            rows[here, n:n + nt] = dot(pack_b, xall[j, :, n:n + nt]).astype(BF16)
        return carry

    def expert_pass(j0, j1, last, hook):
        r0, count = j0 * blk, (j1 - j0) * blk

        def zero(i, carry):
            acc[pl.ds(pl.multiple_of(i * blk, blk), blk), :] = jnp.zeros((blk, d_model), F32)
            return carry

        lax.fori_loop(0, j1 - j0, zero, 0)

        def expert(l, carry):
            slot = l % 2
            hook(l)

            def prefetch():
                for copy in weight_copies((l + 1) % local, (l + 1) % 2):
                    copy.start()

            if last:
                pl.when(l < local - 1)(prefetch)
            else:
                prefetch()
            lane = lax.broadcasted_iota(jnp.int32, (count, local), 1) == l
            pos = jnp.sum(jnp.where(lane, slot_c[r0:r0 + count, :], 0.0), axis=1, keepdims=True)
            gate = jnp.sum(jnp.where(lane, gate_c[r0:r0 + count, :], 0.0), axis=1, keepdims=True)
            fan_t[0:count, :] = jnp.where(pos == lax.broadcasted_iota(jnp.int32, (count, ecap), 1).astype(F32), 1.0, 0.0).astype(BF16)
            row_pos = slot_r[pl.ds(l, 1), r0:r0 + count]
            fan[:, 0:count] = jnp.where(row_pos == lax.broadcasted_iota(jnp.int32, (ecap, count), 0).astype(F32), 1.0, 0.0).astype(BF16)

            for copy in weight_copies(l, slot):
                copy.wait()
            for n in range(0, d_model, nt):
                xin[:, n:n + nt] = dot(fan[:, 0:count], rows[r0:r0 + count, n:n + nt]).astype(BF16)
            for f in range(0, ffn, ft):
                gate_act = dot(xin[...], wgb[slot, :, f:f + ft])
                up_act = dot(xin[...], wub[slot, :, f:f + ft])
                hid[:, f:f + ft] = (jax.nn.silu(gate_act) * up_act).astype(BF16)
            for n in range(0, d_model, nt):
                y = dot(hid[...], wdb[slot, :, n:n + nt]).astype(BF16)
                acc[0:count, n:n + nt] += gate * dot(fan_t[0:count, :], y)
            return carry

        lax.fori_loop(0, local, expert, 0)

        def finish(i, carry):
            rows[pl.ds(pl.multiple_of(r0 + i * blk, blk), blk), :] = acc[pl.ds(pl.multiple_of(i * blk, blk), blk), :].astype(BF16)
            return carry

        lax.fori_loop(0, j1 - j0, finish, 0)

    first, second = 3, split

    def send_back(order):
        for j in order:
            for c in range(2):
                if (j, c) != (0, 0):
                    ret_copy(j, c).start()

    reset_base()
    own_tok.wait()
    wait_sib(0)
    lax.fori_loop(0, 1, pack_slot, 0)
    for j, dev in ((1, right), (2, left)):
        relay_meta(j, j + 2, dev)
    for sub in range(SUBS):
        relay_sub(1, sub, 3, right)
        relay_sub(2, sub, 4, left)
    wait_sib(1)
    wait_sib(2)
    lax.fori_loop(1, first, pack_slot, 0)

    def hook_a(l):
        def meta_step():
            relay_meta(3, 5, right)
            relay_meta(4, 6, left)

        def data_step(sub):
            def step():
                relay_sub(3, sub, 5, right)
                relay_sub(4, sub, 6, left)
            return step

        pl.when(l == 1)(meta_step)
        for sub, at in enumerate((2, 4, 5, 7)):
            pl.when(l == at)(data_step(sub))

    expert_pass(0, first, False, hook_a)
    ret[0:cap, :] = rows[0:cap, :]
    reset_base()
    wait_sib(3)
    wait_sib(4)
    lax.fori_loop(first, second, pack_slot, 0)

    def hook_b(l):
        def meta_step():
            relay_meta(5, far, right)
            relay_meta(6, None, left)

        def data_step(sub):
            def step():
                relay_sub(5, sub, far if sub < SUBS // 2 else None, right)
                relay_sub(6, sub, far if sub >= SUBS // 2 else None, left)
            return step

        pl.when(l == 0)(meta_step)
        for sub, at in enumerate((1, 2, 4, 6)):
            pl.when(l == at)(data_step(sub))
        pl.when(l == 5)(lambda: send_back((1, 2, 0)))

    expert_pass(first, second, False, hook_b)
    send_back((3, 4))
    reset_base()
    wait_sib(5)
    wait_sib(6)
    lax.fori_loop(second, far, pack_slot, 0)
    relay_meta(far, None, right)
    for sub in range(SUBS):
        relay_sub(far, sub, None, right)
    wait_sib(far)
    lax.fori_loop(far, nz, pack_slot, 0)
    expert_pass(second, nz, True, lambda l: None)
    send_back((7, 5, 6))

    near = split * blk
    for j in range(split):
        for c in range(2):
            if (j, c) != (0, 0):
                ret_copy(j, c).wait_recv()

    for n in range(0, d_model, nt):
        acc[0:tok_dev, n:n + nt] = xall[0, 0:tok_dev, n:n + nt].astype(F32) + dot_tn(comb[0:near, :], ret[0:near, n:n + nt])
    for j in range(split, nz):
        for c in range(2):
            ret_copy(j, c).wait_recv()

    for n in range(0, d_model, nt):
        out[:, n:n + nt] = (acc[0:tok_dev, n:n + nt] + dot_tn(comb[near:, :], ret[near:, n:n + nt])).astype(BF16)

    for j in range(nz):
        for i in range(2):
            msib_copy(i, j).wait_send()
            if j > 0:
                mring_copy(i, 0, j, right).wait_send()
        for sub in range(SUBS):
            sib_copy(tok.at[sub_ds(sub)], j, sub).wait_send()
            if j > 0:
                ring_copy(tok.at[sub_ds(sub)], j, sub, right).wait_send()
        for c in range(2):
            if (j, c) != (0, 0):
                ret_copy(j, c).wait_send()


def solution(mesh):
    groups = mesh.shape['ep']
    nz = groups // 2
    row_spec = P(('dp', 'ep'))
    expert_spec = P('ep')

    def device_step(tokens, expert_ids, gate_vals, w_gate, w_up, w_down):
        tok_dev, top_k = expert_ids.shape
        d_model = tokens.shape[1]
        local, _, ffn = w_gate.shape
        cap = tok_dev * (top_k // 2) // groups
        ecap = tok_dev * top_k // local
        row_count = groups * cap
        most = 3 * 2 * cap
        hbm = pl.BlockSpec(memory_space=pl.ANY)
        dma = pltpu.SemaphoreType.DMA
        return pl.pallas_call(
            functools.partial(moe_kernel, groups),
            out_shape=jax.ShapeDtypeStruct(tokens.shape, tokens.dtype),
            in_specs=[hbm] * 6,
            out_specs=pl.BlockSpec(memory_space=pltpu.VMEM),
            scratch_shapes=[
                pltpu.VMEM((nz, 2 * tok_dev, d_model), BF16),
                pltpu.VMEM((nz, top_k, 2 * tok_dev), jnp.int32),
                pltpu.VMEM((nz, top_k, 2 * tok_dev), F32),
                pltpu.VMEM((row_count, d_model), BF16),
                pltpu.VMEM((most, d_model), F32),
                pltpu.VMEM((row_count, d_model), BF16),
                pltpu.VMEM((2, d_model, ffn), BF16),
                pltpu.VMEM((2, d_model, ffn), BF16),
                pltpu.VMEM((2, ffn, d_model), BF16),
                pltpu.VMEM((ecap, d_model), BF16),
                pltpu.VMEM((ecap, ffn), BF16),
                pltpu.VMEM((ecap, most), BF16),
                pltpu.VMEM((most, ecap), BF16),
                pltpu.VMEM((local, row_count), F32),
                pltpu.VMEM((row_count, local), F32),
                pltpu.VMEM((row_count, local), F32),
                pltpu.VMEM((row_count, tok_dev), BF16),
                pltpu.VMEM((tok_dev, tok_dev), BF16),
                pltpu.VMEM((local, 1), F32),
                pltpu.VMEM((1, local), F32),
                dma((nz, SUBS)), dma((nz, SUBS)), dma((nz, SUBS)), dma((nz, SUBS)),
                dma((nz, 2)), dma((nz, 2)), dma((nz, 2)), dma((nz, 2)),
                dma((nz, 2)), dma((nz, 2)), dma((2, 3)), dma((3,)),
            ],
            compiler_params=pltpu.CompilerParams(collective_id=0, has_side_effects=True, vmem_limit_bytes=67043328),
            name='moe_fused',
        )(tokens, expert_ids.T, gate_vals.T, w_gate, w_up, w_down)

    return jax.shard_map(device_step, mesh=mesh, in_specs=(row_spec, row_spec, row_spec, expert_spec, expert_spec, expert_spec), out_specs=row_spec, check_vma=False)
```

```python
import functools

import jax
import jax.numpy as jnp
from jax import lax
from jax.experimental import pallas as pl
from jax.experimental.pallas import tpu as pltpu
from jax.sharding import PartitionSpec as P

MESH = pl.DeviceIdType.MESH
SUBS = 4
F32 = jnp.float32
BF16 = jnp.bfloat16


def dot(a, b):
    return jnp.dot(a, b, preferred_element_type=F32)


def dot_nt(a, b, precision=None):
    return lax.dot_general(a, b, (((1,), (1,)), ((), ())), precision=precision, preferred_element_type=F32)


def dot_tn(a, b):
    return lax.dot_general(a, b, (((0,), (0,)), ((), ())), preferred_element_type=F32)


def moe_kernel(groups, tok, ids_in, gates_in, w_gate, w_up, w_down, out, xall, ids_all, gates_all, rows, acc, ret, wgb, wub, wdb, xin, hid, fan, fan_t,
               slot_r, slot_c, gate_c, comb, tri, base_r, base_c, ring_s, ring_r, sib_s, sib_r, mring_s, mring_r, msib_s, msib_r,
               ret_s, ret_r, wsem, loc):
    nz = groups // 2
    half = nz // 2
    tok_dev, d_model = tok.shape
    local, _, ffn = w_gate.shape
    top_k = ids_in.shape[0]
    cap = tok_dev * (top_k // 2) // groups
    ecap = fan.shape[0]
    sub_rows = tok_dev // SUBS
    blk = 2 * cap
    nt = min(512, d_model)
    ft = min(256, ffn)
    far = nz - 1
    split = 2 * half - 3

    me = lax.axis_index('ep')
    z = me // 2
    k = me % 2
    right = ((z + 1) % nz) * 2 + k
    left = ((z + nz - 1) % nz) * 2 + k
    sib = z * 2 + 1 - k

    def source_shift(j):
        if j == 0:
            return 0
        if j == far:
            return half
        return nz - (j + 1) // 2 if j % 2 == 1 else j // 2

    def device_at(shift, c):
        return ((z + shift) % nz) * 2 + (k if c == 0 else 1 - k)

    def remote(src, dst, ssem, rsem, dev):
        return pltpu.make_async_remote_copy(src_ref=src, dst_ref=dst, send_sem=ssem, recv_sem=rsem, device_id={'ep': dev}, device_id_type=MESH)

    def sub_ds(sub, c=0):
        return pl.ds(c * tok_dev + sub * sub_rows, sub_rows)

    def ring_copy(src, dst_j, sub, dev):
        return remote(src, xall.at[dst_j, sub_ds(sub)], ring_s.at[dst_j, sub], ring_r.at[dst_j, sub], dev)

    def sib_copy(src, j, sub):
        return remote(src, xall.at[j, sub_ds(sub, 1)], sib_s.at[j, sub], sib_r.at[j, sub], sib)

    tables = ((ids_in, ids_all), (gates_in, gates_all))

    def table_src(i, j, own):
        return tables[i][0] if own else tables[i][1].at[j, :, pl.ds(0, tok_dev)]

    def mring_copy(i, src_j, dst_j, dev):
        return remote(table_src(i, src_j, src_j == 0), tables[i][1].at[dst_j, :, pl.ds(0, tok_dev)], mring_s.at[dst_j, i], mring_r.at[dst_j, i], dev)

    def msib_copy(i, j):
        return remote(table_src(i, j, j == 0), tables[i][1].at[j, :, pl.ds(tok_dev, tok_dev)], msib_s.at[j, i], msib_r.at[j, i], sib)

    def ret_copy(j, c):
        off = j * blk + c * cap
        return remote(rows.at[pl.ds(off, cap)], ret.at[pl.ds(off, cap)], ret_s.at[j, c], ret_r.at[j, c], device_at(source_shift(j), c))

    def weight_copies(expert, slot):
        return (pltpu.make_async_copy(w_gate.at[expert], wgb.at[slot], wsem.at[slot, 0]),
                pltpu.make_async_copy(w_up.at[expert], wub.at[slot], wsem.at[slot, 1]),
                pltpu.make_async_copy(w_down.at[expert], wdb.at[slot], wsem.at[slot, 2]))

    own_tok = pltpu.make_async_copy(tok, xall.at[0, pl.ds(0, tok_dev)], loc.at[0])
    own_tables = [pltpu.make_async_copy(tables[i][0], tables[i][1].at[0, :, pl.ds(0, tok_dev)], loc.at[1 + i]) for i in range(2)]
    for copy in own_tables:
        copy.start()
    own_tok.start()

    barrier = pltpu.get_barrier_semaphore()
    for step in range(1, groups):
        pl.semaphore_signal(barrier, inc=1, device_id={'ep': (me + step) % groups}, device_id_type=MESH)
    pl.semaphore_wait(barrier, groups - 1)

    for i in range(2):
        mring_copy(i, 0, 1, right).start()
        mring_copy(i, 0, 2, left).start()
        msib_copy(i, 0).start()
    for sub in range(SUBS):
        ring_copy(tok.at[sub_ds(sub)], 1, sub, right).start()
        ring_copy(tok.at[sub_ds(sub)], 2, sub, left).start()
    for sub in range(SUBS):
        sib_copy(tok.at[sub_ds(sub)], 0, sub).start()
    for copy in weight_copies(0, 0):
        copy.start()

    def relay_meta(j, next_j, dev):
        for i in range(2):
            mring_copy(i, j, j, dev).wait_recv()
            if next_j is not None:
                mring_copy(i, j, next_j, dev).start()
            msib_copy(i, j).start()

    def relay_sub(j, sub, next_j, dev):
        here = xall.at[j, sub_ds(sub)]
        ring_copy(here, j, sub, dev).wait_recv()
        if next_j is not None:
            ring_copy(here, next_j, sub, dev).start()
        sib_copy(here, j, sub).start()

    def wait_sib(j):
        for i in range(2):
            msib_copy(i, j).wait_recv()
        for sub in range(SUBS):
            sib_copy(xall.at[j, sub_ds(sub)], j, sub).wait_recv()

    tok_row = lax.broadcasted_iota(jnp.int32, (tok_dev, tok_dev), 0)
    tok_col = lax.broadcasted_iota(jnp.int32, (tok_dev, tok_dev), 1)
    tri[...] = jnp.where(tok_row < tok_col, 1.0, 0.0).astype(BF16)

    for copy in own_tables:
        copy.wait()
    row_id = lax.broadcasted_iota(jnp.int32, (2 * nz, tok_dev), 0)
    peer_lo = jnp.zeros((2 * nz, tok_dev), jnp.int32)
    for j in range(nz):
        for c in range(2):
            peer = device_at((nz - source_shift(j)) % nz, c)
            peer_lo = jnp.where(row_id == 2 * j + c, peer * local, peer_lo)
    own_ids = ids_all[0, :, 0:tok_dev]
    picked = jnp.zeros((2 * nz, tok_dev), F32)
    for i in range(top_k):
        rel = own_ids[i:i + 1, :] - peer_lo
        picked = jnp.where((rel >= 0) & (rel < local), 1.0, picked)
    rank = jnp.where(picked > 0, dot(picked.astype(BF16), tri[...]), -1.0)
    cap_iota = lax.broadcasted_iota(jnp.int32, (cap, tok_dev), 0).astype(F32)
    for r in range(2 * nz):
        comb[r * cap:(r + 1) * cap, :] = jnp.where(rank[r:r + 1, :] == cap_iota, 1.0, 0.0).astype(BF16)

    lo = me * local

    def reset_base():
        base_r[...] = jnp.zeros_like(base_r)
        base_c[...] = jnp.zeros_like(base_c)

    def pack_slot(j, carry):
        gts = gates_all[j]
        rel = ids_all[j] - lo
        chosen = jnp.max(jnp.where((rel >= 0) & (rel < local), 1.0, 0.0), axis=0, keepdims=True)
        halves = []
        for c in range(2):
            ch = jnp.broadcast_to(chosen[:, c * tok_dev:(c + 1) * tok_dev], (8, tok_dev)).astype(BF16)
            halves.append(dot(ch, tri[...])[0:1, :] + float(c * cap))
        rank2 = jnp.where(chosen > 0, jnp.concatenate(halves, axis=1), -1.0)
        pack = jnp.where(rank2 == lax.broadcasted_iota(jnp.int32, (blk, 2 * tok_dev), 0).astype(F32), 1.0, 0.0)
        pack_b = pack.astype(BF16)
        loc_iota = lax.broadcasted_iota(jnp.int32, (local, 2 * tok_dev), 0)
        mem = jnp.zeros((local, 2 * tok_dev), F32)
        gat = jnp.zeros((local, 2 * tok_dev), F32)
        for i in range(top_k):
            hit = rel[i:i + 1, :] == loc_iota
            mem = jnp.where(hit, 1.0, mem)
            gat = jnp.where(hit, gts[i:i + 1, :], gat)
        mem_b = mem.astype(BF16)
        mem_r = dot_nt(mem_b, pack_b)
        mem_c = dot_nt(pack_b, mem_b)
        gate_j = dot_nt(pack, gat, lax.Precision.HIGHEST)
        tri_b = tri[0:blk, 0:blk]
        pos_r = dot(mem_r.astype(BF16), tri_b) + base_r[...]
        pos_c = dot_tn(tri_b, mem_c.astype(BF16)) + base_c[...]
        here = pl.ds(pl.multiple_of(j * blk, blk), blk)
        slot_r[:, here] = jnp.where(mem_r > 0, pos_r, -1.0)
        slot_c[here, :] = jnp.where(mem_c > 0, pos_c, -1.0)
        gate_c[here, :] = gate_j
        base_r[...] += jnp.sum(mem_r, axis=1, keepdims=True)
        base_c[...] += jnp.sum(mem_c, axis=0, keepdims=True)

        for n in range(0, d_model, nt):
            rows[here, n:n + nt] = dot(pack_b, xall[j, :, n:n + nt]).astype(BF16)
        return carry

    def expert_pass(j0, j1, last, hook):
        r0, count = j0 * blk, (j1 - j0) * blk

        def zero(i, carry):
            acc[pl.ds(pl.multiple_of(i * blk, blk), blk), :] = jnp.zeros((blk, d_model), F32)
            return carry

        lax.fori_loop(0, j1 - j0, zero, 0)

        def gather(l):
            row_pos = slot_r[pl.ds(l, 1), r0:r0 + count]
            fan[:, 0:count] = jnp.where(row_pos == lax.broadcasted_iota(jnp.int32, (ecap, count), 0).astype(F32), 1.0, 0.0).astype(BF16)
            for n in range(0, d_model, nt):
                xin[:, n:n + nt] = dot(fan[:, 0:count], rows[r0:r0 + count, n:n + nt]).astype(BF16)

        def expert(l, carry):
            slot = l % 2
            hook(l)

            def prefetch():
                for copy in weight_copies((l + 1) % local, (l + 1) % 2):
                    copy.start()

            if last:
                pl.when(l < local - 1)(prefetch)
            else:
                prefetch()
            for copy in weight_copies(l, slot):
                copy.wait()
            for f in range(0, ffn, ft):
                gate_act = dot(xin[...], wgb[slot, :, f:f + ft])
                up_act = dot(xin[...], wub[slot, :, f:f + ft])
                hid[:, f:f + ft] = (jax.nn.silu(gate_act) * up_act).astype(BF16)
            gather((l + 1) % local)
            lane = lax.broadcasted_iota(jnp.int32, (count, local), 1) == l
            pos = jnp.sum(jnp.where(lane, slot_c[r0:r0 + count, :], 0.0), axis=1, keepdims=True)
            gate = jnp.sum(jnp.where(lane, gate_c[r0:r0 + count, :], 0.0), axis=1, keepdims=True)
            fan_t[0:count, :] = jnp.where(pos == lax.broadcasted_iota(jnp.int32, (count, ecap), 1).astype(F32), 1.0, 0.0).astype(BF16)

            def spread(n, y):
                acc[0:count, n:n + nt] += gate * dot(fan_t[0:count, :], y)

            held = None
            for n in range(0, d_model, nt):
                y = dot(hid[...], wdb[slot, :, n:n + nt]).astype(BF16)
                if held is not None:
                    spread(*held)
                held = (n, y)
            spread(*held)
            return carry

        gather(0)
        lax.fori_loop(0, local, expert, 0)

        def finish(i, carry):
            rows[pl.ds(pl.multiple_of(r0 + i * blk, blk), blk), :] = acc[pl.ds(pl.multiple_of(i * blk, blk), blk), :].astype(BF16)
            return carry

        lax.fori_loop(0, j1 - j0, finish, 0)

    first, second = 3, split

    def send_back(order):
        for j in order:
            for c in range(2):
                if (j, c) != (0, 0):
                    ret_copy(j, c).start()

    reset_base()
    own_tok.wait()
    wait_sib(0)
    lax.fori_loop(0, 1, pack_slot, 0)
    for j, dev in ((1, right), (2, left)):
        relay_meta(j, j + 2, dev)
    for sub in range(SUBS):
        relay_sub(1, sub, 3, right)
        relay_sub(2, sub, 4, left)
    wait_sib(1)
    wait_sib(2)
    lax.fori_loop(1, first, pack_slot, 0)

    def hook_a(l):
        def meta_step():
            relay_meta(3, 5, right)
            relay_meta(4, 6, left)

        def data_step(sub):
            def step():
                relay_sub(3, sub, 5, right)
                relay_sub(4, sub, 6, left)
            return step

        pl.when(l == 1)(meta_step)
        for sub, at in enumerate((2, 4, 5, 7)):
            pl.when(l == at)(data_step(sub))

    expert_pass(0, first, False, hook_a)
    ret[0:cap, :] = rows[0:cap, :]
    reset_base()
    wait_sib(3)
    wait_sib(4)
    lax.fori_loop(first, second, pack_slot, 0)

    def hook_b(l):
        def meta_step():
            relay_meta(5, far, right)
            relay_meta(6, None, left)

        def data_step(sub):
            def step():
                relay_sub(5, sub, far if sub < SUBS // 2 else None, right)
                relay_sub(6, sub, far if sub >= SUBS // 2 else None, left)
            return step

        pl.when(l == 0)(meta_step)
        for sub, at in enumerate((1, 2, 4, 6)):
            pl.when(l == at)(data_step(sub))
        pl.when(l == 5)(lambda: send_back((1, 2, 0)))

    expert_pass(first, second, False, hook_b)
    send_back((3, 4))
    reset_base()
    wait_sib(5)
    wait_sib(6)
    lax.fori_loop(second, far, pack_slot, 0)
    relay_meta(far, None, right)
    for sub in range(SUBS):
        relay_sub(far, sub, None, right)
    wait_sib(far)
    lax.fori_loop(far, nz, pack_slot, 0)
    expert_pass(second, nz, True, lambda l: None)
    send_back((7, 5, 6))

    near = split * blk
    for j in range(split):
        for c in range(2):
            if (j, c) != (0, 0):
                ret_copy(j, c).wait_recv()

    for n in range(0, d_model, nt):
        acc[0:tok_dev, n:n + nt] = xall[0, 0:tok_dev, n:n + nt].astype(F32) + dot_tn(comb[0:near, :], ret[0:near, n:n + nt])
    for j in range(split, nz):
        for c in range(2):
            ret_copy(j, c).wait_recv()

    for n in range(0, d_model, nt):
        out[:, n:n + nt] = (acc[0:tok_dev, n:n + nt] + dot_tn(comb[near:, :], ret[near:, n:n + nt])).astype(BF16)

    for j in range(nz):
        for i in range(2):
            msib_copy(i, j).wait_send()
            if j > 0:
                mring_copy(i, 0, j, right).wait_send()
        for sub in range(SUBS):
            sib_copy(tok.at[sub_ds(sub)], j, sub).wait_send()
            if j > 0:
                ring_copy(tok.at[sub_ds(sub)], j, sub, right).wait_send()
        for c in range(2):
            if (j, c) != (0, 0):
                ret_copy(j, c).wait_send()


def solution(mesh):
    groups = mesh.shape['ep']
    nz = groups // 2
    row_spec = P(('dp', 'ep'))
    expert_spec = P('ep')

    def device_step(tokens, expert_ids, gate_vals, w_gate, w_up, w_down):
        tok_dev, top_k = expert_ids.shape
        d_model = tokens.shape[1]
        local, _, ffn = w_gate.shape
        cap = tok_dev * (top_k // 2) // groups
        ecap = tok_dev * top_k // local
        row_count = groups * cap
        most = 3 * 2 * cap
        hbm = pl.BlockSpec(memory_space=pl.ANY)
        dma = pltpu.SemaphoreType.DMA
        return pl.pallas_call(
            functools.partial(moe_kernel, groups),
            out_shape=jax.ShapeDtypeStruct(tokens.shape, tokens.dtype),
            in_specs=[hbm] * 6,
            out_specs=pl.BlockSpec(memory_space=pltpu.VMEM),
            scratch_shapes=[
                pltpu.VMEM((nz, 2 * tok_dev, d_model), BF16),
                pltpu.VMEM((nz, top_k, 2 * tok_dev), jnp.int32),
                pltpu.VMEM((nz, top_k, 2 * tok_dev), F32),
                pltpu.VMEM((row_count, d_model), BF16),
                pltpu.VMEM((most, d_model), F32),
                pltpu.VMEM((row_count, d_model), BF16),
                pltpu.VMEM((2, d_model, ffn), BF16),
                pltpu.VMEM((2, d_model, ffn), BF16),
                pltpu.VMEM((2, ffn, d_model), BF16),
                pltpu.VMEM((ecap, d_model), BF16),
                pltpu.VMEM((ecap, ffn), BF16),
                pltpu.VMEM((ecap, most), BF16),
                pltpu.VMEM((most, ecap), BF16),
                pltpu.VMEM((local, row_count), F32),
                pltpu.VMEM((row_count, local), F32),
                pltpu.VMEM((row_count, local), F32),
                pltpu.VMEM((row_count, tok_dev), BF16),
                pltpu.VMEM((tok_dev, tok_dev), BF16),
                pltpu.VMEM((local, 1), F32),
                pltpu.VMEM((1, local), F32),
                dma((nz, SUBS)), dma((nz, SUBS)), dma((nz, SUBS)), dma((nz, SUBS)),
                dma((nz, 2)), dma((nz, 2)), dma((nz, 2)), dma((nz, 2)),
                dma((nz, 2)), dma((nz, 2)), dma((2, 3)), dma((3,)),
            ],
            compiler_params=pltpu.CompilerParams(collective_id=0, has_side_effects=True, vmem_limit_bytes=67043328),
            name='moe_fused',
        )(tokens, expert_ids.T, gate_vals.T, w_gate, w_up, w_down)

    return jax.shard_map(device_step, mesh=mesh, in_specs=(row_spec, row_spec, row_spec, expert_spec, expert_spec, expert_spec), out_specs=row_spec, check_vma=False)
```

```python
import functools

import jax
import jax.numpy as jnp
from jax import lax
from jax.experimental import pallas as pl
from jax.experimental.pallas import tpu as pltpu
from jax.sharding import PartitionSpec as P

MESH = pl.DeviceIdType.MESH
SUBS = 4
F32 = jnp.float32
BF16 = jnp.bfloat16


def dot(a, b):
    return jnp.dot(a, b, preferred_element_type=F32)


def dot_nt(a, b, precision=None):
    return lax.dot_general(a, b, (((1,), (1,)), ((), ())), precision=precision, preferred_element_type=F32)


def dot_tn(a, b):
    return lax.dot_general(a, b, (((0,), (0,)), ((), ())), preferred_element_type=F32)


def moe_kernel(groups, tok, ids_in, gates_in, w_gate, w_up, w_down, out, xall, ids_all, gates_all, rows, acc, ret, wgb, wub, wdb, xin, hid, fan, fan_t,
               slot_r, slot_c, gate_c, comb, tri, base_r, base_c, packs, ring_s, ring_r, sib_s, sib_r, mring_s, mring_r, msib_s, msib_r,
               ret_s, ret_r, wsem, loc):
    nz = groups // 2
    half = nz // 2
    tok_dev, d_model = tok.shape
    local, _, ffn = w_gate.shape
    top_k = ids_in.shape[0]
    cap = tok_dev * (top_k // 2) // groups
    ecap = fan.shape[0]
    sub_rows = tok_dev // SUBS
    blk = 2 * cap
    nt = min(512, d_model)
    ft = min(256, ffn)
    far = nz - 1
    split = 2 * half - 3

    me = lax.axis_index('ep')
    z = me // 2
    k = me % 2
    right = ((z + 1) % nz) * 2 + k
    left = ((z + nz - 1) % nz) * 2 + k
    sib = z * 2 + 1 - k

    def source_shift(j):
        if j == 0:
            return 0
        if j == far:
            return half
        return nz - (j + 1) // 2 if j % 2 == 1 else j // 2

    def device_at(shift, c):
        return ((z + shift) % nz) * 2 + (k if c == 0 else 1 - k)

    def remote(src, dst, ssem, rsem, dev):
        return pltpu.make_async_remote_copy(src_ref=src, dst_ref=dst, send_sem=ssem, recv_sem=rsem, device_id={'ep': dev}, device_id_type=MESH)

    def sub_ds(sub, c=0):
        return pl.ds(c * tok_dev + sub * sub_rows, sub_rows)

    def swing(i):
        return (i + SUBS // 2) % SUBS

    def ring_copy(src, dst_j, sub, dev):
        return remote(src, xall.at[dst_j, sub_ds(sub)], ring_s.at[dst_j, sub], ring_r.at[dst_j, sub], dev)

    def sib_copy(src, j, sub):
        return remote(src, xall.at[j, sub_ds(sub, 1)], sib_s.at[j, sub], sib_r.at[j, sub], sib)

    tables = ((ids_in, ids_all), (gates_in, gates_all))

    def table_src(i, j, own):
        return tables[i][0] if own else tables[i][1].at[j, :, pl.ds(0, tok_dev)]

    def mring_copy(i, src_j, dst_j, dev):
        return remote(table_src(i, src_j, src_j == 0), tables[i][1].at[dst_j, :, pl.ds(0, tok_dev)], mring_s.at[dst_j, i], mring_r.at[dst_j, i], dev)

    def msib_copy(i, j):
        return remote(table_src(i, j, j == 0), tables[i][1].at[j, :, pl.ds(tok_dev, tok_dev)], msib_s.at[j, i], msib_r.at[j, i], sib)

    def ret_copy(j, c):
        off = j * blk + c * cap
        return remote(rows.at[pl.ds(off, cap)], ret.at[pl.ds(off, cap)], ret_s.at[j, c], ret_r.at[j, c], device_at(source_shift(j), c))

    def weight_copies(expert, slot):
        return (pltpu.make_async_copy(w_gate.at[expert], wgb.at[slot], wsem.at[slot, 0]),
                pltpu.make_async_copy(w_up.at[expert], wub.at[slot], wsem.at[slot, 1]),
                pltpu.make_async_copy(w_down.at[expert], wdb.at[slot], wsem.at[slot, 2]))

    own_tok = pltpu.make_async_copy(tok, xall.at[0, pl.ds(0, tok_dev)], loc.at[0])
    own_tables = [pltpu.make_async_copy(tables[i][0], tables[i][1].at[0, :, pl.ds(0, tok_dev)], loc.at[1 + i]) for i in range(2)]
    for copy in own_tables:
        copy.start()
    own_tok.start()

    barrier = pltpu.get_barrier_semaphore()
    for step in range(1, groups):
        pl.semaphore_signal(barrier, inc=1, device_id={'ep': (me + step) % groups}, device_id_type=MESH)
    pl.semaphore_wait(barrier, groups - 1)

    for i in range(2):
        mring_copy(i, 0, 1, right).start()
        mring_copy(i, 0, 2, left).start()
        msib_copy(i, 0).start()
    for i in range(SUBS):
        ring_copy(tok.at[sub_ds(i)], 1, i, right).start()
        ring_copy(tok.at[sub_ds(swing(i))], 2, swing(i), left).start()
    for sub in range(SUBS):
        sib_copy(tok.at[sub_ds(sub)], 0, sub).start()
    for copy in weight_copies(0, 0):
        copy.start()

    def relay_meta(j, next_j, dev):
        for i in range(2):
            mring_copy(i, j, j, dev).wait_recv()
            if next_j is not None:
                mring_copy(i, j, next_j, dev).start()
            msib_copy(i, j).start()

    def relay_sub(j, sub, next_j, dev):
        here = xall.at[j, sub_ds(sub)]
        ring_copy(here, j, sub, dev).wait_recv()
        if next_j is not None:
            ring_copy(here, next_j, sub, dev).start()
        sib_copy(here, j, sub).start()

    def wait_sib_tables(j):
        for i in range(2):
            msib_copy(i, j).wait_recv()

    def wait_sib(j):
        for sub in range(SUBS):
            sib_copy(xall.at[j, sub_ds(sub)], j, sub).wait_recv()

    tok_row = lax.broadcasted_iota(jnp.int32, (tok_dev, tok_dev), 0)
    tok_col = lax.broadcasted_iota(jnp.int32, (tok_dev, tok_dev), 1)
    tri[...] = jnp.where(tok_row < tok_col, 1.0, 0.0).astype(BF16)

    for copy in own_tables:
        copy.wait()
    row_id = lax.broadcasted_iota(jnp.int32, (2 * nz, tok_dev), 0)
    peer_lo = jnp.zeros((2 * nz, tok_dev), jnp.int32)
    for j in range(nz):
        for c in range(2):
            peer = device_at((nz - source_shift(j)) % nz, c)
            peer_lo = jnp.where(row_id == 2 * j + c, peer * local, peer_lo)
    own_ids = ids_all[0, :, 0:tok_dev]
    picked = jnp.zeros((2 * nz, tok_dev), F32)
    for i in range(top_k):
        rel = own_ids[i:i + 1, :] - peer_lo
        picked = jnp.where((rel >= 0) & (rel < local), 1.0, picked)
    rank = jnp.where(picked > 0, dot(picked.astype(BF16), tri[...]), -1.0)
    cap_iota = lax.broadcasted_iota(jnp.int32, (cap, tok_dev), 0).astype(F32)
    for r in range(2 * nz):
        comb[r * cap:(r + 1) * cap, :] = jnp.where(rank[r:r + 1, :] == cap_iota, 1.0, 0.0).astype(BF16)

    lo = me * local

    def reset_base():
        base_r[...] = jnp.zeros_like(base_r)
        base_c[...] = jnp.zeros_like(base_c)

    def slot_tables(j, carry):
        gts = gates_all[j]
        rel = ids_all[j] - lo
        chosen = jnp.max(jnp.where((rel >= 0) & (rel < local), 1.0, 0.0), axis=0, keepdims=True)
        halves = []
        for c in range(2):
            ch = jnp.broadcast_to(chosen[:, c * tok_dev:(c + 1) * tok_dev], (8, tok_dev)).astype(BF16)
            halves.append(dot(ch, tri[...])[0:1, :] + float(c * cap))
        rank2 = jnp.where(chosen > 0, jnp.concatenate(halves, axis=1), -1.0)
        pack = jnp.where(rank2 == lax.broadcasted_iota(jnp.int32, (blk, 2 * tok_dev), 0).astype(F32), 1.0, 0.0)
        pack_b = pack.astype(BF16)
        loc_iota = lax.broadcasted_iota(jnp.int32, (local, 2 * tok_dev), 0)
        mem = jnp.zeros((local, 2 * tok_dev), F32)
        gat = jnp.zeros((local, 2 * tok_dev), F32)
        for i in range(top_k):
            hit = rel[i:i + 1, :] == loc_iota
            mem = jnp.where(hit, 1.0, mem)
            gat = jnp.where(hit, gts[i:i + 1, :], gat)
        mem_b = mem.astype(BF16)
        mem_r = dot_nt(mem_b, pack_b)
        mem_c = dot_nt(pack_b, mem_b)
        gate_j = dot_nt(pack, gat, lax.Precision.HIGHEST)
        tri_b = tri[0:blk, 0:blk]
        pos_r = dot(mem_r.astype(BF16), tri_b) + base_r[...]
        pos_c = dot_tn(tri_b, mem_c.astype(BF16)) + base_c[...]
        here = pl.ds(pl.multiple_of(j * blk, blk), blk)
        slot_r[:, here] = jnp.where(mem_r > 0, pos_r, -1.0)
        slot_c[here, :] = jnp.where(mem_c > 0, pos_c, -1.0)
        gate_c[here, :] = gate_j
        base_r[...] += jnp.sum(mem_r, axis=1, keepdims=True)
        base_c[...] += jnp.sum(mem_c, axis=0, keepdims=True)

        packs[j % 3] = pack_b
        return carry

    def pack_rows(j, carry):
        here = pl.ds(pl.multiple_of(j * blk, blk), blk)
        for n in range(0, d_model, nt):
            rows[here, n:n + nt] = dot(packs[j % 3], xall[j, :, n:n + nt]).astype(BF16)
        return carry

    def gather(l, a, b, add):
        lo_r, hi_r = a * blk, b * blk
        wide = hi_r - lo_r
        row_pos = slot_r[pl.ds(l, 1), lo_r:hi_r]
        fan[:, 0:wide] = jnp.where(row_pos == lax.broadcasted_iota(jnp.int32, (ecap, wide), 0).astype(F32), 1.0, 0.0).astype(BF16)
        for n in range(0, d_model, nt):
            got = dot(fan[:, 0:wide], rows[lo_r:hi_r, n:n + nt])
            if add:
                got = got + xin[l, :, n:n + nt].astype(F32)
            xin[l, :, n:n + nt] = got.astype(BF16)

    def expert_pass(j0, j1, g0, last, hook):
        r0, count = j0 * blk, (j1 - j0) * blk

        def zero(i, carry):
            acc[pl.ds(pl.multiple_of(i * blk, blk), blk), :] = jnp.zeros((blk, d_model), F32)
            return carry

        lax.fori_loop(0, j1 - j0, zero, 0)

        def expert(l, carry):
            slot = l % 2
            hook(l)

            def prefetch():
                for copy in weight_copies((l + 1) % local, (l + 1) % 2):
                    copy.start()

            if last:
                pl.when(l < local - 1)(prefetch)
            else:
                prefetch()
            for copy in weight_copies(l, slot):
                copy.wait()
            for f in range(0, ffn, ft):
                gate_act = dot(xin[l], wgb[slot, :, f:f + ft])
                up_act = dot(xin[l], wub[slot, :, f:f + ft])
                hid[:, f:f + ft] = (jax.nn.silu(gate_act) * up_act).astype(BF16)
            gather((l + 1) % local, g0, j1, g0 != j0)
            lane = lax.broadcasted_iota(jnp.int32, (count, local), 1) == l
            pos = jnp.sum(jnp.where(lane, slot_c[r0:r0 + count, :], 0.0), axis=1, keepdims=True)
            gate = jnp.sum(jnp.where(lane, gate_c[r0:r0 + count, :], 0.0), axis=1, keepdims=True)
            fan_t[0:count, :] = jnp.where(pos == lax.broadcasted_iota(jnp.int32, (count, ecap), 1).astype(F32), 1.0, 0.0).astype(BF16)

            def spread(n, y):
                acc[0:count, n:n + nt] += gate * dot(fan_t[0:count, :], y)

            held = None
            for n in range(0, d_model, nt):
                y = dot(hid[...], wdb[slot, :, n:n + nt]).astype(BF16)
                if held is not None:
                    spread(*held)
                held = (n, y)
            spread(*held)
            return carry

        gather(0, g0, j1, g0 != j0)
        lax.fori_loop(0, local, expert, 0)

        def finish(i, carry):
            rows[pl.ds(pl.multiple_of(r0 + i * blk, blk), blk), :] = acc[pl.ds(pl.multiple_of(i * blk, blk), blk), :].astype(BF16)
            return carry

        lax.fori_loop(0, j1 - j0, finish, 0)

    first, second = 3, split

    def send_back(order):
        for j in order:
            for c in range(2):
                if (j, c) != (0, 0):
                    ret_copy(j, c).start()

    def send_back(order):
        for j in order:
            for c in range(2):
                if (j, c) != (0, 0):
                    ret_copy(j, c).start()

    reset_base()
    wait_sib_tables(0)
    lax.fori_loop(0, 1, slot_tables, 0)
    own_tok.wait()
    wait_sib(0)
    lax.fori_loop(0, 1, pack_rows, 0)
    for s in range(1, half - 1):
        jr, jl = 2 * s - 1, 2 * s
        relay_meta(jr, jr + 2, right)
        relay_meta(jl, jl + 2, left)
        wait_sib_tables(jr)
        wait_sib_tables(jl)
        lax.fori_loop(jr, jl + 1, slot_tables, 0)
        for i in range(SUBS):
            relay_sub(jr, i, jr + 2, right)
            relay_sub(jl, swing(i), jl + 2, left)
        wait_sib(jr)
        wait_sib(jl)
        lax.fori_loop(jr, jl + 1, pack_rows, 0)
        if s == half - 3:
            def early(l, carry):
                gather(l, 0, jl + 1, False)
                return carry

            lax.fori_loop(0, local, early, 0)
            reached = jl + 1

    jr, jl = split, split + 1

    def hook_a(l):
        def meta_step():
            relay_meta(jr, far, right)
            relay_meta(jl, None, left)

        def data_step(i):
            def step():
                relay_sub(jr, i, far if i < SUBS // 2 else None, right)
                relay_sub(jl, swing(i), far if i < SUBS // 2 else None, left)
            return step

        pl.when(l == 0)(meta_step)
        for i, at in enumerate((1, 2, 4, 5)):
            pl.when(l == at)(data_step(i))

    expert_pass(0, split, reached, False, hook_a)
    ret[0:cap, :] = rows[0:cap, :]
    send_back(range(split - 1, -1, -1))
    reset_base()
    relay_meta(far, None, right)
    for j in range(split, nz):
        wait_sib_tables(j)
    lax.fori_loop(split, nz, slot_tables, 0)
    wait_sib(jr)
    wait_sib(jl)
    lax.fori_loop(split, far, pack_rows, 0)
    for sub in range(SUBS):
        relay_sub(far, sub, None, right)
    wait_sib(far)
    lax.fori_loop(far, nz, pack_rows, 0)
    expert_pass(split, nz, split, True, lambda l: None)
    send_back(range(nz - 1, split - 1, -1))

    near = split * blk
    for j in range(split):
        for c in range(2):
            if (j, c) != (0, 0):
                ret_copy(j, c).wait_recv()

    for n in range(0, d_model, nt):
        acc[0:tok_dev, n:n + nt] = xall[0, 0:tok_dev, n:n + nt].astype(F32) + dot_tn(comb[0:near, :], ret[0:near, n:n + nt])
    for j in range(split, nz):
        for c in range(2):
            ret_copy(j, c).wait_recv()

    for n in range(0, d_model, nt):
        out[:, n:n + nt] = (acc[0:tok_dev, n:n + nt] + dot_tn(comb[near:, :], ret[near:, n:n + nt])).astype(BF16)

    for j in range(nz):
        for i in range(2):
            msib_copy(i, j).wait_send()
            if j > 0:
                mring_copy(i, 0, j, right).wait_send()
        for sub in range(SUBS):
            sib_copy(tok.at[sub_ds(sub)], j, sub).wait_send()
            if j > 0:
                ring_copy(tok.at[sub_ds(sub)], j, sub, right).wait_send()
        for c in range(2):
            if (j, c) != (0, 0):
                ret_copy(j, c).wait_send()


def solution(mesh):
    groups = mesh.shape['ep']
    nz = groups // 2
    row_spec = P(('dp', 'ep'))
    expert_spec = P('ep')

    def device_step(tokens, expert_ids, gate_vals, w_gate, w_up, w_down):
        tok_dev, top_k = expert_ids.shape
        d_model = tokens.shape[1]
        local, _, ffn = w_gate.shape
        cap = tok_dev * (top_k // 2) // groups
        ecap = tok_dev * top_k // local
        row_count = groups * cap
        most = (2 * (nz // 2) - 3) * 2 * cap
        hbm = pl.BlockSpec(memory_space=pl.ANY)
        dma = pltpu.SemaphoreType.DMA
        return pl.pallas_call(
            functools.partial(moe_kernel, groups),
            out_shape=jax.ShapeDtypeStruct(tokens.shape, tokens.dtype),
            in_specs=[hbm] * 6,
            out_specs=pl.BlockSpec(memory_space=pltpu.VMEM),
            scratch_shapes=[
                pltpu.VMEM((nz, 2 * tok_dev, d_model), BF16),
                pltpu.VMEM((nz, top_k, 2 * tok_dev), jnp.int32),
                pltpu.VMEM((nz, top_k, 2 * tok_dev), F32),
                pltpu.VMEM((row_count, d_model), BF16),
                pltpu.VMEM((most, d_model), F32),
                pltpu.VMEM((row_count, d_model), BF16),
                pltpu.VMEM((2, d_model, ffn), BF16),
                pltpu.VMEM((2, d_model, ffn), BF16),
                pltpu.VMEM((2, ffn, d_model), BF16),
                pltpu.VMEM((local, ecap, d_model), BF16),
                pltpu.VMEM((ecap, ffn), BF16),
                pltpu.VMEM((ecap, most), BF16),
                pltpu.VMEM((most, ecap), BF16),
                pltpu.VMEM((local, row_count), F32),
                pltpu.VMEM((row_count, local), F32),
                pltpu.VMEM((row_count, local), F32),
                pltpu.VMEM((row_count, tok_dev), BF16),
                pltpu.VMEM((tok_dev, tok_dev), BF16),
                pltpu.VMEM((local, 1), F32),
                pltpu.VMEM((1, local), F32),
                pltpu.VMEM((3, 2 * cap, 2 * tok_dev), BF16),
                dma((nz, SUBS)), dma((nz, SUBS)), dma((nz, SUBS)), dma((nz, SUBS)),
                dma((nz, 2)), dma((nz, 2)), dma((nz, 2)), dma((nz, 2)),
                dma((nz, 2)), dma((nz, 2)), dma((2, 3)), dma((3,)),
            ],
            compiler_params=pltpu.CompilerParams(collective_id=0, has_side_effects=True, vmem_limit_bytes=67043328),
            name='moe_fused',
        )(tokens, expert_ids.T, gate_vals.T, w_gate, w_up, w_down)

    return jax.shard_map(device_step, mesh=mesh, in_specs=(row_spec, row_spec, row_spec, expert_spec, expert_spec, expert_spec), out_specs=row_spec, check_vma=False)
```

```python
import functools

import jax
import jax.numpy as jnp
from jax import lax
from jax.experimental import pallas as pl
from jax.experimental.pallas import tpu as pltpu
from jax.sharding import PartitionSpec as P

MESH = pl.DeviceIdType.MESH
SUBS = 4
F32 = jnp.float32
BF16 = jnp.bfloat16


def dot(a, b):
    return jnp.dot(a, b, preferred_element_type=F32)


def dot_nt(a, b, precision=None):
    return lax.dot_general(a, b, (((1,), (1,)), ((), ())), precision=precision, preferred_element_type=F32)


def dot_tn(a, b):
    return lax.dot_general(a, b, (((0,), (0,)), ((), ())), preferred_element_type=F32)


def moe_kernel(groups, tok, ids_in, gates_in, w_gate, w_up, w_down, out, xall, ids_all, gates_all, rows, acc, total, ret, wgb, wub, wdb, xin, hid, fan, fan_t,
               slot_r, slot_c, gate_c, comb, tri, base_r, base_c, packs, ship, sends, ring_s, ring_r, sib_s, sib_r, mring_s, mring_r, msib_s, msib_r,
               far_s, far_r, ret_s, ret_r, wsem, dsem, loc):
    nz = groups // 2
    half = nz // 2
    tok_dev, d_model = tok.shape
    local, _, ffn = w_gate.shape
    top_k = ids_in.shape[0]
    cap = tok_dev * (top_k // 2) // groups
    ecap = fan.shape[0]
    sub_rows = tok_dev // SUBS
    blk = 2 * cap
    cuts = 4
    nt = d_model // cuts
    ft = min(256, ffn)
    far = nz - 1
    split = 2 * half - 3

    me = lax.axis_index('ep')
    z = me // 2
    k = me % 2
    right = ((z + 1) % nz) * 2 + k
    left = ((z + nz - 1) % nz) * 2 + k
    sib = z * 2 + 1 - k

    def source_shift(j):
        if j == 0:
            return 0
        if j == far:
            return half
        return nz - (j + 1) // 2 if j % 2 == 1 else j // 2

    def device_at(shift, c):
        return ((z + shift) % nz) * 2 + (k if c == 0 else 1 - k)

    def remote(src, dst, ssem, rsem, dev):
        return pltpu.make_async_remote_copy(src_ref=src, dst_ref=dst, send_sem=ssem, recv_sem=rsem, device_id={'ep': dev}, device_id_type=MESH)

    def sub_ds(sub, c=0):
        return pl.ds(c * tok_dev + sub * sub_rows, sub_rows)

    def swing(i):
        return (i + SUBS // 2) % SUBS

    def ring_copy(src, dst_j, sub, dev):
        return remote(src, xall.at[dst_j, sub_ds(sub)], ring_s.at[dst_j, sub], ring_r.at[dst_j, sub], dev)

    def sib_copy(src, j, sub):
        return remote(src, xall.at[j, sub_ds(sub, 1)], sib_s.at[j, sub], sib_r.at[j, sub], sib)

    tables = ((ids_in, ids_all), (gates_in, gates_all))

    def table_src(i, j, own):
        return tables[i][0] if own else tables[i][1].at[j, :, pl.ds(0, tok_dev)]

    def mring_copy(i, src_j, dst_j, dev):
        return remote(table_src(i, src_j, src_j == 0), tables[i][1].at[dst_j, :, pl.ds(0, tok_dev)], mring_s.at[dst_j, i], mring_r.at[dst_j, i], dev)

    def msib_copy(i, j):
        return remote(table_src(i, j, j == 0), tables[i][1].at[j, :, pl.ds(tok_dev, tok_dev)], msib_s.at[j, i], msib_r.at[j, i], sib)

    def columns(m):
        return pl.ds(pl.multiple_of(m * nt, nt), nt)

    def ret_copy(j, c, m):
        part = (pl.ds(j * blk + c * cap, cap), columns(m))
        return remote(rows.at[part], ret.at[part], ret_s.at[j, c, m], ret_r.at[j, c, m], device_at(source_shift(j), c))

    def far_copy(side, i):
        j, c = ((split, 0), (split, 1), (far, 0))[i] if side == 0 else ((split + 1, 0), (split + 1, 1), (far, 1))[i]
        shift = (1, 1, 2)[i] if side == 0 else (nz - 1, nz - 1, nz - 2)[i]
        core = (0, 1, side)[i]
        src = sends.at[side, pl.ds(i * cap, cap)]
        return remote(src, rows.at[pl.ds(j * blk + c * cap, cap)], far_s.at[side, i], far_r.at[side, i], device_at(shift, core))

    def weight_copies(expert, slot):
        return (pltpu.make_async_copy(w_gate.at[expert], wgb.at[slot], wsem.at[slot, 0]),
                pltpu.make_async_copy(w_up.at[expert], wub.at[slot], wsem.at[slot, 1]))

    def down_tile(l, bank):
        if bank == 0:
            return wdb.at[l // 4, :, pl.ds((l % 4) * nt, nt)]
        buf = wgb if l < 4 else wub
        return buf.at[(l % 4) // 2, pl.ds((l % 2) * ffn, ffn), pl.ds(0, nt)]

    def down_copies(m, bank):
        return [pltpu.make_async_copy(w_down.at[l, :, columns(m)], down_tile(l, bank), dsem.at[bank, l]) for l in range(local)]

    own_tok = pltpu.make_async_copy(tok, xall.at[0, pl.ds(0, tok_dev)], loc.at[0])
    own_tables = [pltpu.make_async_copy(tables[i][0], tables[i][1].at[0, :, pl.ds(0, tok_dev)], loc.at[1 + i]) for i in range(2)]
    for copy in own_tables:
        copy.start()
    own_tok.start()

    barrier = pltpu.get_barrier_semaphore()
    for step in range(1, groups):
        pl.semaphore_signal(barrier, inc=1, device_id={'ep': (me + step) % groups}, device_id_type=MESH)
    pl.semaphore_wait(barrier, groups - 1)

    for i in range(2):
        mring_copy(i, 0, 1, right).start()
        mring_copy(i, 0, 2, left).start()
        msib_copy(i, 0).start()
    for i in range(SUBS):
        ring_copy(tok.at[sub_ds(i)], 1, i, right).start()
        ring_copy(tok.at[sub_ds(swing(i))], 2, swing(i), left).start()
    for sub in range(SUBS):
        sib_copy(tok.at[sub_ds(sub)], 0, sub).start()
    for copy in weight_copies(0, 0):
        copy.start()

    def relay_meta(j, next_j, dev):
        for i in range(2):
            mring_copy(i, j, j, dev).wait_recv()
            if next_j is not None:
                mring_copy(i, j, next_j, dev).start()
            msib_copy(i, j).start()

    def relay_sub(j, sub, next_j, dev):
        here = xall.at[j, sub_ds(sub)]
        ring_copy(here, j, sub, dev).wait_recv()
        if next_j is not None:
            ring_copy(here, next_j, sub, dev).start()
        sib_copy(here, j, sub).start()

    def wait_sib_tables(j):
        for i in range(2):
            msib_copy(i, j).wait_recv()

    def wait_sib(j):
        for sub in range(SUBS):
            sib_copy(xall.at[j, sub_ds(sub)], j, sub).wait_recv()

    tok_row = lax.broadcasted_iota(jnp.int32, (tok_dev, tok_dev), 0)
    tok_col = lax.broadcasted_iota(jnp.int32, (tok_dev, tok_dev), 1)
    tri[...] = jnp.where(tok_row < tok_col, 1.0, 0.0).astype(BF16)

    for copy in own_tables:
        copy.wait()
    row_id = lax.broadcasted_iota(jnp.int32, (2 * nz, tok_dev), 0)
    peer_lo = jnp.zeros((2 * nz, tok_dev), jnp.int32)
    for j in range(nz):
        for c in range(2):
            peer = device_at((nz - source_shift(j)) % nz, c)
            peer_lo = jnp.where(row_id == 2 * j + c, peer * local, peer_lo)
    own_ids = ids_all[0, :, 0:tok_dev]
    picked = jnp.zeros((2 * nz, tok_dev), F32)
    for i in range(top_k):
        rel = own_ids[i:i + 1, :] - peer_lo
        picked = jnp.where((rel >= 0) & (rel < local), 1.0, picked)
    rank = jnp.where(picked > 0, dot(picked.astype(BF16), tri[...]), -1.0)
    cap_iota = lax.broadcasted_iota(jnp.int32, (cap, tok_dev), 0).astype(F32)
    for r in range(2 * nz):
        comb[r * cap:(r + 1) * cap, :] = jnp.where(rank[r:r + 1, :] == cap_iota, 1.0, 0.0).astype(BF16)

    lo = me * local

    def reset_base():
        base_r[...] = jnp.zeros_like(base_r)
        base_c[...] = jnp.zeros_like(base_c)

    def slot_tables(j, carry):
        gts = gates_all[j]
        rel = ids_all[j] - lo
        chosen = jnp.max(jnp.where((rel >= 0) & (rel < local), 1.0, 0.0), axis=0, keepdims=True)
        halves = []
        for c in range(2):
            ch = jnp.broadcast_to(chosen[:, c * tok_dev:(c + 1) * tok_dev], (8, tok_dev)).astype(BF16)
            halves.append(dot(ch, tri[...])[0:1, :] + float(c * cap))
        rank2 = jnp.where(chosen > 0, jnp.concatenate(halves, axis=1), -1.0)
        pack = jnp.where(rank2 == lax.broadcasted_iota(jnp.int32, (blk, 2 * tok_dev), 0).astype(F32), 1.0, 0.0)
        pack_b = pack.astype(BF16)
        loc_iota = lax.broadcasted_iota(jnp.int32, (local, 2 * tok_dev), 0)
        mem = jnp.zeros((local, 2 * tok_dev), F32)
        gat = jnp.zeros((local, 2 * tok_dev), F32)
        for i in range(top_k):
            hit = rel[i:i + 1, :] == loc_iota
            mem = jnp.where(hit, 1.0, mem)
            gat = jnp.where(hit, gts[i:i + 1, :], gat)
        mem_b = mem.astype(BF16)
        mem_r = dot_nt(mem_b, pack_b)
        mem_c = dot_nt(pack_b, mem_b)
        gate_j = dot_nt(pack, gat, lax.Precision.HIGHEST)
        tri_b = tri[0:blk, 0:blk]
        pos_r = dot(mem_r.astype(BF16), tri_b) + base_r[...]
        pos_c = dot_tn(tri_b, mem_c.astype(BF16)) + base_c[...]
        here = pl.ds(pl.multiple_of(j * blk, blk), blk)
        slot_r[:, here] = jnp.where(mem_r > 0, pos_r, -1.0)
        slot_c[here, :] = jnp.where(mem_c > 0, pos_c, -1.0)
        gate_c[here, :] = gate_j
        base_r[...] += jnp.sum(mem_r, axis=1, keepdims=True)
        base_c[...] += jnp.sum(mem_c, axis=0, keepdims=True)

        packs[j % 3] = pack_b
        return carry

    def pack_rows(j, carry):
        here = pl.ds(pl.multiple_of(j * blk, blk), blk)
        for n in range(0, d_model, nt):
            rows[here, n:n + nt] = dot(packs[j % 3], xall[j, :, n:n + nt]).astype(BF16)
        return carry

    def gather(l, a, b, add):
        lo_r, hi_r = a * blk, b * blk
        wide = hi_r - lo_r
        row_pos = slot_r[pl.ds(l, 1), lo_r:hi_r]
        fan[:, 0:wide] = jnp.where(row_pos == lax.broadcasted_iota(jnp.int32, (ecap, wide), 0).astype(F32), 1.0, 0.0).astype(BF16)
        for n in range(0, d_model, nt):
            got = dot(fan[:, 0:wide], rows[lo_r:hi_r, n:n + nt])
            if add:
                got = got + xin[l, :, n:n + nt].astype(F32)
            xin[l, :, n:n + nt] = got.astype(BF16)

    def expert_pass(j0, j1, g0, hook, order):
        r0, count = j0 * blk, (j1 - j0) * blk
        for copy in down_copies(0, 0):
            copy.start()
        gather(0, g0, j1, g0 != j0)

        def expert(l, carry):
            slot = l % 2
            hook(l)

            def prefetch():
                for copy in weight_copies(l + 1, (l + 1) % 2):
                    copy.start()

            pl.when(l < local - 1)(prefetch)
            for copy in weight_copies(l, slot):
                copy.wait()
            for f in range(0, ffn, ft):
                gate_act = dot(xin[l], wgb[slot, :, f:f + ft])
                up_act = dot(xin[l], wub[slot, :, f:f + ft])
                hid[l, :, f:f + ft] = (jax.nn.silu(gate_act) * up_act).astype(BF16)
            gather((l + 1) % local, g0, j1, g0 != j0)
            lane = lax.broadcasted_iota(jnp.int32, (count, local), 1) == l
            pos = jnp.sum(jnp.where(lane, slot_c[r0:r0 + count, :], 0.0), axis=1, keepdims=True)
            fan_t[l, 0:count, :] = jnp.where(pos == lax.broadcasted_iota(jnp.int32, (count, ecap), 1).astype(F32), 1.0, 0.0).astype(BF16)
            return carry

        lax.fori_loop(0, local, expert, 0)

        def column(m, bank):
            for copy in down_copies(m, bank):
                copy.wait()

            def spread(l, y):
                part = gate_c[r0:r0 + count, l:l + 1] * dot(fan_t[l, 0:count, :], y)
                if l == 0:
                    acc[0:count, :] = part
                else:
                    acc[0:count, :] += part

            held = None
            for l in range(local):
                tile = wdb[l // 4, :, (l % 4) * nt:(l % 4 + 1) * nt] if bank == 0 else (wgb if l < 4 else wub)[(l % 4) // 2, (l % 2) * ffn:(l % 2 + 1) * ffn, 0:nt]
                y = dot(hid[l], tile).astype(BF16)
                if held is not None:
                    spread(*held)
                held = (l, y)
            spread(*held)
            rows[r0:r0 + count, columns(m)] = acc[0:count, :].astype(BF16)
            if j0 == 0:
                ret[0:cap, columns(m)] = acc[0:cap, :].astype(BF16)
            for j in order:
                for c in range(2):
                    if (j, c) != (0, 0):
                        ret_copy(j, c, m).start()

        def two_columns(i, carry):
            for copy in down_copies(2 * i + 1, 1):
                copy.start()
            column(2 * i, 0)

            def prefetch():
                for copy in down_copies(2 * i + 2, 0):
                    copy.start()

            pl.when(i < cuts // 2 - 1)(prefetch)
            column(2 * i + 1, 1)
            return carry

        lax.fori_loop(0, cuts // 2, two_columns, 0)

    def ship_tables(side, j):
        ids = ids_all[j, :, 0:tok_dev]
        row_id = lax.broadcasted_iota(jnp.int32, (8, tok_dev), 0)
        peers = [device_at(shift, core) for shift, core in (((1, 0), (1, 1), (2, 0)) if side == 0 else ((nz - 1, 0), (nz - 1, 1), (nz - 2, 1)))]
        low = jnp.full((8, tok_dev), groups * local, jnp.int32)
        for i, peer in enumerate(peers):
            low = jnp.where(row_id == i, peer * local, low)
        took = jnp.zeros((8, tok_dev), F32)
        for i in range(top_k):
            rel = ids[i:i + 1, :] - low
            took = jnp.where((rel >= 0) & (rel < local), 1.0, took)
        place = jnp.where(took > 0, dot(took.astype(BF16), tri[...]), -1.0)
        for i in range(3):
            ship[side, i * cap:(i + 1) * cap, :] = jnp.where(place[i:i + 1, :] == cap_iota, 1.0, 0.0).astype(BF16)

    def ship_rows(side, j):
        for n in range(0, d_model, nt):
            sends[side, :, n:n + nt] = dot(ship[side], xall[j, 0:tok_dev, n:n + nt]).astype(BF16)
        for i in range(3):
            far_copy(side, i).start()

    reset_base()
    wait_sib_tables(0)
    lax.fori_loop(0, 1, slot_tables, 0)
    own_tok.wait()
    wait_sib(0)
    lax.fori_loop(0, 1, pack_rows, 0)
    for s in range(1, half - 1):
        jr, jl = 2 * s - 1, 2 * s
        relay_meta(jr, jr + 2, right)
        relay_meta(jl, jl + 2, left)
        wait_sib_tables(jr)
        wait_sib_tables(jl)
        lax.fori_loop(jr, jl + 1, slot_tables, 0)
        onward = s < half - 2
        if not onward:
            ship_tables(0, jr)
            ship_tables(1, jl)
        for i in range(SUBS):
            relay_sub(jr, i, jr + 2 if onward else None, right)
            relay_sub(jl, swing(i), jl + 2 if onward else None, left)
        if not onward:
            ship_rows(0, jr)
            ship_rows(1, jl)
        wait_sib(jr)
        wait_sib(jl)
        lax.fori_loop(jr, jl + 1, pack_rows, 0)
        if s == half - 3:
            def early(l, carry):
                gather(l, 0, jl + 1, False)
                return carry

            lax.fori_loop(0, local, early, 0)
            reached = jl + 1

    jr, jl = split, split + 1

    def hook_a(l):
        def meta_step():
            relay_meta(jr, far, right)
            relay_meta(jl, None, left)

        pl.when(l == 0)(meta_step)

    expert_pass(0, split, reached, hook_a, range(split - 1, -1, -1))
    for copy in weight_copies(0, 0):
        copy.start()
    reset_base()
    relay_meta(far, None, right)
    for j in range(split, nz):
        wait_sib_tables(j)
    lax.fori_loop(split, nz, slot_tables, 0)
    for side in range(2):
        for i in range(3):
            far_copy(side, i).wait_recv()
    expert_pass(split, nz, split, lambda l: None, range(nz - 1, split - 1, -1))

    near = split * blk
    for m in range(cuts):
        for j in range(split):
            for c in range(2):
                if (j, c) != (0, 0):
                    ret_copy(j, c, m).wait_recv()
        n = m * nt
        total[:, n:n + nt] = xall[0, 0:tok_dev, n:n + nt].astype(F32) + dot_tn(comb[0:near, :], ret[0:near, n:n + nt])
    for m in range(cuts):
        for j in range(split, nz):
            for c in range(2):
                ret_copy(j, c, m).wait_recv()
        n = m * nt
        out[:, n:n + nt] = (total[:, n:n + nt] + dot_tn(comb[near:, :], ret[near:, n:n + nt])).astype(BF16)

    for side in range(2):
        for i in range(3):
            far_copy(side, i).wait_send()
    for j in range(nz):
        for i in range(2):
            msib_copy(i, j).wait_send()
            if j > 0:
                mring_copy(i, 0, j, right).wait_send()
        if j < split:
            for sub in range(SUBS):
                sib_copy(tok.at[sub_ds(sub)], j, sub).wait_send()
                if j > 0:
                    ring_copy(tok.at[sub_ds(sub)], j, sub, right).wait_send()
        for c in range(2):
            for m in range(cuts):
                if (j, c) != (0, 0):
                    ret_copy(j, c, m).wait_send()


def solution(mesh):
    groups = mesh.shape['ep']
    nz = groups // 2
    row_spec = P(('dp', 'ep'))
    expert_spec = P('ep')

    def device_step(tokens, expert_ids, gate_vals, w_gate, w_up, w_down):
        tok_dev, top_k = expert_ids.shape
        d_model = tokens.shape[1]
        local, _, ffn = w_gate.shape
        cap = tok_dev * (top_k // 2) // groups
        ecap = tok_dev * top_k // local
        row_count = groups * cap
        most = (2 * (nz // 2) - 3) * 2 * cap
        hbm = pl.BlockSpec(memory_space=pl.ANY)
        dma = pltpu.SemaphoreType.DMA
        return pl.pallas_call(
            functools.partial(moe_kernel, groups),
            out_shape=jax.ShapeDtypeStruct(tokens.shape, tokens.dtype),
            in_specs=[hbm] * 6,
            out_specs=pl.BlockSpec(memory_space=pltpu.VMEM),
            scratch_shapes=[
                pltpu.VMEM((2 * (nz // 2) - 3, 2 * tok_dev, d_model), BF16),
                pltpu.VMEM((nz, top_k, 2 * tok_dev), jnp.int32),
                pltpu.VMEM((nz, top_k, 2 * tok_dev), F32),
                pltpu.VMEM((row_count, d_model), BF16),
                pltpu.VMEM((most, d_model // 4), F32),
                pltpu.VMEM((tok_dev, d_model), F32),
                pltpu.VMEM((row_count, d_model), BF16),
                pltpu.VMEM((2, d_model, ffn), BF16),
                pltpu.VMEM((2, d_model, ffn), BF16),
                pltpu.VMEM((2, ffn, d_model), BF16),
                pltpu.VMEM((local, ecap, d_model), BF16),
                pltpu.VMEM((local, ecap, ffn), BF16),
                pltpu.VMEM((ecap, most), BF16),
                pltpu.VMEM((local, most, ecap), BF16),
                pltpu.VMEM((local, row_count), F32),
                pltpu.VMEM((row_count, local), F32),
                pltpu.VMEM((row_count, local), F32),
                pltpu.VMEM((row_count, tok_dev), BF16),
                pltpu.VMEM((tok_dev, tok_dev), BF16),
                pltpu.VMEM((local, 1), F32),
                pltpu.VMEM((1, local), F32),
                pltpu.VMEM((3, 2 * cap, 2 * tok_dev), BF16),
                pltpu.VMEM((2, 3 * cap, tok_dev), BF16),
                pltpu.VMEM((2, 3 * cap, d_model), BF16),
                dma((nz, SUBS)), dma((nz, SUBS)), dma((nz, SUBS)), dma((nz, SUBS)),
                dma((nz, 2)), dma((nz, 2)), dma((nz, 2)), dma((nz, 2)),
                dma((2, 3)), dma((2, 3)), dma((nz, 2, 4)), dma((nz, 2, 4)), dma((2, 2)), dma((2, local)), dma((3,)),
            ],
            compiler_params=pltpu.CompilerParams(collective_id=0, has_side_effects=True, vmem_limit_bytes=67043328),
            name='moe_fused',
        )(tokens, expert_ids.T, gate_vals.T, w_gate, w_up, w_down)

    return jax.shard_map(device_step, mesh=mesh, in_specs=(row_spec, row_spec, row_spec, expert_spec, expert_spec, expert_spec), out_specs=row_spec, check_vma=False)
```

```python
import functools

import jax
import jax.numpy as jnp
from jax import lax
from jax.experimental import pallas as pl
from jax.experimental.pallas import tpu as pltpu
from jax.sharding import PartitionSpec as P

MESH = pl.DeviceIdType.MESH
SUBS = 4
F32 = jnp.float32
BF16 = jnp.bfloat16


def dot(a, b):
    return jnp.dot(a, b, preferred_element_type=F32)


def dot_nt(a, b, precision=None):
    return lax.dot_general(a, b, (((1,), (1,)), ((), ())), precision=precision, preferred_element_type=F32)


def dot_tn(a, b):
    return lax.dot_general(a, b, (((0,), (0,)), ((), ())), preferred_element_type=F32)


def moe_kernel(groups, tok, ids_in, gates_in, w_gate, w_up, w_down, out, xall, ids_all, gates_all, rows, acc, ret, wgb, wub, wdb, xin, hid, fan, fan_t,
               slot_r, slot_c, gate_c, comb, tri, base_r, base_c, packs, ship, sends, ring_s, ring_r, sib_s, sib_r, mring_s, mring_r, msib_s, msib_r,
               far_s, far_r, ret_s, ret_r, wsem, dsem, loc):
    nz = groups // 2
    half = nz // 2
    tok_dev, d_model = tok.shape
    local, _, ffn = w_gate.shape
    top_k = ids_in.shape[0]
    cap = tok_dev * (top_k // 2) // groups
    ecap = fan.shape[0]
    sub_rows = tok_dev // SUBS
    blk = 2 * cap
    cuts = 4
    nt = d_model // cuts
    ft = min(256, ffn)
    far = nz - 1
    split = 2 * half - 3

    me = lax.axis_index('ep')
    z = me // 2
    k = me % 2
    right = ((z + 1) % nz) * 2 + k
    left = ((z + nz - 1) % nz) * 2 + k
    sib = z * 2 + 1 - k

    def source_shift(j):
        if j == 0:
            return 0
        if j == far:
            return half
        return nz - (j + 1) // 2 if j % 2 == 1 else j // 2

    def device_at(shift, c):
        return ((z + shift) % nz) * 2 + (k if c == 0 else 1 - k)

    def remote(src, dst, ssem, rsem, dev):
        return pltpu.make_async_remote_copy(src_ref=src, dst_ref=dst, send_sem=ssem, recv_sem=rsem, device_id={'ep': dev}, device_id_type=MESH)

    def sub_ds(sub, c=0):
        return pl.ds(c * tok_dev + sub * sub_rows, sub_rows)

    def swing(i):
        return (i + SUBS // 2) % SUBS

    def ring_copy(src, dst_j, sub, dev):
        return remote(src, xall.at[dst_j, sub_ds(sub)], ring_s.at[dst_j, sub], ring_r.at[dst_j, sub], dev)

    def sib_copy(src, j, sub):
        return remote(src, xall.at[j, sub_ds(sub, 1)], sib_s.at[j, sub], sib_r.at[j, sub], sib)

    tables = ((ids_in, ids_all), (gates_in, gates_all))

    def table_src(i, j, own):
        return tables[i][0] if own else tables[i][1].at[j, :, pl.ds(0, tok_dev)]

    def mring_copy(i, src_j, dst_j, dev):
        return remote(table_src(i, src_j, src_j == 0), tables[i][1].at[dst_j, :, pl.ds(0, tok_dev)], mring_s.at[dst_j, i], mring_r.at[dst_j, i], dev)

    def msib_copy(i, j):
        return remote(table_src(i, j, j == 0), tables[i][1].at[j, :, pl.ds(tok_dev, tok_dev)], msib_s.at[j, i], msib_r.at[j, i], sib)

    def columns(m):
        return pl.ds(pl.multiple_of(m * nt, nt), nt)

    def ret_copy(j, c, m):
        part = (pl.ds(j * blk + c * cap, cap), columns(m))
        return remote(rows.at[part], ret.at[part], ret_s.at[j, c, m], ret_r.at[j, c, m], device_at(source_shift(j), c))

    def far_copy(side, i):
        j, c = ((split, 0), (split, 1), (far, 0))[i] if side == 0 else ((split + 1, 0), (split + 1, 1), (far, 1))[i]
        shift = (1, 1, 2)[i] if side == 0 else (nz - 1, nz - 1, nz - 2)[i]
        core = (0, 1, side)[i]
        src = sends.at[side, pl.ds(i * cap, cap)]
        return remote(src, rows.at[pl.ds(j * blk + c * cap, cap)], far_s.at[side, i], far_r.at[side, i], device_at(shift, core))

    def weight_copies(expert, slot):
        return (pltpu.make_async_copy(w_gate.at[expert], wgb.at[slot], wsem.at[slot, 0]),
                pltpu.make_async_copy(w_up.at[expert], wub.at[slot], wsem.at[slot, 1]))

    def down_tile(l, bank):
        if bank == 0:
            return wdb.at[l // 4, :, pl.ds((l % 4) * nt, nt)]
        buf = wgb if l < 4 else wub
        return buf.at[(l % 4) // 2, pl.ds((l % 2) * ffn, ffn), pl.ds(0, nt)]

    def down_copies(m, bank):
        return [pltpu.make_async_copy(w_down.at[l, :, columns(m)], down_tile(l, bank), dsem.at[bank, l]) for l in range(local)]

    own_tok = pltpu.make_async_copy(tok, xall.at[0, pl.ds(0, tok_dev)], loc.at[0])
    own_tables = [pltpu.make_async_copy(tables[i][0], tables[i][1].at[0, :, pl.ds(0, tok_dev)], loc.at[1 + i]) for i in range(2)]
    for copy in own_tables:
        copy.start()
    own_tok.start()

    barrier = pltpu.get_barrier_semaphore()
    for step in range(1, groups):
        pl.semaphore_signal(barrier, inc=1, device_id={'ep': (me + step) % groups}, device_id_type=MESH)
    pl.semaphore_wait(barrier, groups - 1)

    for i in range(2):
        mring_copy(i, 0, 1, right).start()
        mring_copy(i, 0, 2, left).start()
        msib_copy(i, 0).start()
    for i in range(SUBS):
        ring_copy(tok.at[sub_ds(i)], 1, i, right).start()
        ring_copy(tok.at[sub_ds(swing(i))], 2, swing(i), left).start()
    for sub in range(SUBS):
        sib_copy(tok.at[sub_ds(sub)], 0, sub).start()
    for expert in range(3):
        for copy in weight_copies(expert, (expert + 2) % 3):
            copy.start()

    def relay_meta(j, next_j, dev):
        for i in range(2):
            mring_copy(i, j, j, dev).wait_recv()
            if next_j is not None:
                mring_copy(i, j, next_j, dev).start()
            msib_copy(i, j).start()

    def relay_sub(j, sub, next_j, dev):
        here = xall.at[j, sub_ds(sub)]
        ring_copy(here, j, sub, dev).wait_recv()
        if next_j is not None:
            ring_copy(here, next_j, sub, dev).start()
        sib_copy(here, j, sub).start()

    def wait_sib_tables(j):
        for i in range(2):
            msib_copy(i, j).wait_recv()

    def wait_sib(j):
        for sub in range(SUBS):
            sib_copy(xall.at[j, sub_ds(sub)], j, sub).wait_recv()

    tok_row = lax.broadcasted_iota(jnp.int32, (tok_dev, tok_dev), 0)
    tok_col = lax.broadcasted_iota(jnp.int32, (tok_dev, tok_dev), 1)
    tri[...] = jnp.where(tok_row < tok_col, 1.0, 0.0).astype(BF16)

    for copy in own_tables:
        copy.wait()
    row_id = lax.broadcasted_iota(jnp.int32, (2 * nz, tok_dev), 0)
    peer_lo = jnp.zeros((2 * nz, tok_dev), jnp.int32)
    for j in range(nz):
        for c in range(2):
            peer = device_at((nz - source_shift(j)) % nz, c)
            peer_lo = jnp.where(row_id == 2 * j + c, peer * local, peer_lo)
    own_ids = ids_all[0, :, 0:tok_dev]
    picked = jnp.zeros((2 * nz, tok_dev), F32)
    for i in range(top_k):
        rel = own_ids[i:i + 1, :] - peer_lo
        picked = jnp.where((rel >= 0) & (rel < local), 1.0, picked)
    rank = jnp.where(picked > 0, dot(picked.astype(BF16), tri[...]), -1.0)
    cap_iota = lax.broadcasted_iota(jnp.int32, (cap, tok_dev), 0).astype(F32)
    for r in range(2 * nz):
        comb[r * cap:(r + 1) * cap, :] = jnp.where(rank[r:r + 1, :] == cap_iota, 1.0, 0.0).astype(BF16)

    lo = me * local

    def reset_base():
        base_r[...] = jnp.zeros_like(base_r)
        base_c[...] = jnp.zeros_like(base_c)

    def slot_tables(j, carry):
        gts = gates_all[j]
        rel = ids_all[j] - lo
        chosen = jnp.max(jnp.where((rel >= 0) & (rel < local), 1.0, 0.0), axis=0, keepdims=True)
        halves = []
        for c in range(2):
            ch = jnp.broadcast_to(chosen[:, c * tok_dev:(c + 1) * tok_dev], (8, tok_dev)).astype(BF16)
            halves.append(dot(ch, tri[...])[0:1, :] + float(c * cap))
        rank2 = jnp.where(chosen > 0, jnp.concatenate(halves, axis=1), -1.0)
        pack = jnp.where(rank2 == lax.broadcasted_iota(jnp.int32, (blk, 2 * tok_dev), 0).astype(F32), 1.0, 0.0)
        pack_b = pack.astype(BF16)
        loc_iota = lax.broadcasted_iota(jnp.int32, (local, 2 * tok_dev), 0)
        mem = jnp.zeros((local, 2 * tok_dev), F32)
        gat = jnp.zeros((local, 2 * tok_dev), F32)
        for i in range(top_k):
            hit = rel[i:i + 1, :] == loc_iota
            mem = jnp.where(hit, 1.0, mem)
            gat = jnp.where(hit, gts[i:i + 1, :], gat)
        mem_b = mem.astype(BF16)
        mem_r = dot_nt(mem_b, pack_b)
        mem_c = dot_nt(pack_b, mem_b)
        gate_j = dot_nt(pack, gat, lax.Precision.HIGHEST)
        tri_b = tri[0:blk, 0:blk]
        pos_r = dot(mem_r.astype(BF16), tri_b) + base_r[...]
        pos_c = dot_tn(tri_b, mem_c.astype(BF16)) + base_c[...]
        here = pl.ds(pl.multiple_of(j * blk, blk), blk)
        slot_r[:, here] = jnp.where(mem_r > 0, pos_r, -1.0)
        slot_c[here, :] = jnp.where(mem_c > 0, pos_c, -1.0)
        gate_c[here, :] = gate_j
        base_r[...] += jnp.sum(mem_r, axis=1, keepdims=True)
        base_c[...] += jnp.sum(mem_c, axis=0, keepdims=True)

        packs[j % 3] = pack_b
        return carry

    def pack_rows(j, carry):
        here = pl.ds(pl.multiple_of(j * blk, blk), blk)
        for n in range(0, d_model, nt):
            rows[here, n:n + nt] = dot(packs[j % 3], xall[j, :, n:n + nt]).astype(BF16)
        return carry

    def gather(l, a, b, add):
        lo_r, hi_r = a * blk, b * blk
        wide = hi_r - lo_r
        row_pos = slot_r[pl.ds(l, 1), lo_r:hi_r]
        fan[:, 0:wide] = jnp.where(row_pos == lax.broadcasted_iota(jnp.int32, (ecap, wide), 0).astype(F32), 1.0, 0.0).astype(BF16)
        for n in range(0, d_model, nt):
            got = dot(fan[:, 0:wide], rows[lo_r:hi_r, n:n + nt])
            if add:
                got = got + xin[l, :, n:n + nt].astype(F32)
            xin[l, :, n:n + nt] = got.astype(BF16)

    def expert_pass(j0, j1, g0, last, hook, order):
        r0, count = j0 * blk, (j1 - j0) * blk
        for copy in down_copies(0, 0):
            copy.start()
        gather(0, g0, j1, g0 != j0)

        def expert(l, carry):
            slot = (l + 2) % 3
            hook(l)

            def prefetch():
                for copy in weight_copies(l + 2, (l + 1) % 3):
                    copy.start()

            def prefetch_next_pass():
                for copy in weight_copies(0, 2):
                    copy.start()

            pl.when((l > 0) & (l < local - 2))(prefetch)
            if not last:
                pl.when(l == local - 1)(prefetch_next_pass)
            for copy in weight_copies(l, slot):
                copy.wait()
            for f in range(0, ffn, ft):
                gate_act = dot(xin[l], wgb[slot, :, f:f + ft])
                up_act = dot(xin[l], wub[slot, :, f:f + ft])
                hid[l, :, f:f + ft] = (jax.nn.silu(gate_act) * up_act).astype(BF16)
            gather((l + 1) % local, g0, j1, g0 != j0)
            lane = lax.broadcasted_iota(jnp.int32, (count, local), 1) == l
            pos = jnp.sum(jnp.where(lane, slot_c[r0:r0 + count, :], 0.0), axis=1, keepdims=True)
            fan_t[l, 0:count, :] = jnp.where(pos == lax.broadcasted_iota(jnp.int32, (count, ecap), 1).astype(F32), 1.0, 0.0).astype(BF16)
            return carry

        lax.fori_loop(0, local, expert, 0)

        def column(m, bank):
            for copy in down_copies(m, bank):
                copy.wait()

            def spread(l, y):
                part = gate_c[r0:r0 + count, l:l + 1] * dot(fan_t[l, 0:count, :], y)
                if l == 0:
                    acc[0:count, :] = part
                else:
                    acc[0:count, :] += part

            held = None
            for l in range(local):
                tile = wdb[l // 4, :, (l % 4) * nt:(l % 4 + 1) * nt] if bank == 0 else (wgb if l < 4 else wub)[(l % 4) // 2, (l % 2) * ffn:(l % 2 + 1) * ffn, 0:nt]
                y = dot(hid[l], tile).astype(BF16)
                if held is not None:
                    spread(*held)
                held = (l, y)
            spread(*held)
            rows[r0:r0 + count, columns(m)] = acc[0:count, :].astype(BF16)
            if j0 == 0:
                ret[0:cap, columns(m)] = acc[0:cap, :].astype(BF16)
            for j in order:
                for c in range(2):
                    if (j, c) != (0, 0):
                        ret_copy(j, c, m).start()

        def two_columns(i, carry):
            for copy in down_copies(2 * i + 1, 1):
                copy.start()
            column(2 * i, 0)

            def prefetch():
                for copy in down_copies(2 * i + 2, 0):
                    copy.start()

            pl.when(i < cuts // 2 - 1)(prefetch)
            column(2 * i + 1, 1)
            return carry

        lax.fori_loop(0, cuts // 2, two_columns, 0)

    def ship_tables(side, j):
        ids = ids_all[j, :, 0:tok_dev]
        row_id = lax.broadcasted_iota(jnp.int32, (8, tok_dev), 0)
        peers = [device_at(shift, core) for shift, core in (((1, 0), (1, 1), (2, 0)) if side == 0 else ((nz - 1, 0), (nz - 1, 1), (nz - 2, 1)))]
        low = jnp.full((8, tok_dev), groups * local, jnp.int32)
        for i, peer in enumerate(peers):
            low = jnp.where(row_id == i, peer * local, low)
        took = jnp.zeros((8, tok_dev), F32)
        for i in range(top_k):
            rel = ids[i:i + 1, :] - low
            took = jnp.where((rel >= 0) & (rel < local), 1.0, took)
        place = jnp.where(took > 0, dot(took.astype(BF16), tri[...]), -1.0)
        for i in range(3):
            ship[side, i * cap:(i + 1) * cap, :] = jnp.where(place[i:i + 1, :] == cap_iota, 1.0, 0.0).astype(BF16)

    def ship_rows(side, j):
        for n in range(0, d_model, nt):
            sends[side, :, n:n + nt] = dot(ship[side], xall[j, 0:tok_dev, n:n + nt]).astype(BF16)
        for i in range(3):
            far_copy(side, i).start()

    reset_base()
    wait_sib_tables(0)
    lax.fori_loop(0, 1, slot_tables, 0)
    own_tok.wait()
    wait_sib(0)
    lax.fori_loop(0, 1, pack_rows, 0)
    for s in range(1, half - 1):
        jr, jl = 2 * s - 1, 2 * s
        relay_meta(jr, jr + 2, right)
        relay_meta(jl, jl + 2, left)
        wait_sib_tables(jr)
        wait_sib_tables(jl)
        lax.fori_loop(jr, jl + 1, slot_tables, 0)
        onward = s < half - 2
        if not onward:
            ship_tables(0, jr)
            ship_tables(1, jl)
        for i in range(SUBS):
            relay_sub(jr, i, jr + 2 if onward else None, right)
            relay_sub(jl, swing(i), jl + 2 if onward else None, left)
        if not onward:
            ship_rows(0, jr)
            ship_rows(1, jl)
        wait_sib(jr)
        wait_sib(jl)
        lax.fori_loop(jr, jl + 1, pack_rows, 0)
        if s == half - 3:
            def early(l, carry):
                gather(l, 0, jl + 1, False)
                return carry

            lax.fori_loop(0, local, early, 0)
            reached = jl + 1

    jr, jl = split, split + 1

    def hook_a(l):
        def meta_step():
            relay_meta(jr, far, right)
            relay_meta(jl, None, left)

        pl.when(l == 0)(meta_step)

    expert_pass(0, split, reached, False, hook_a, range(split - 1, -1, -1))
    for expert in (1, 2):
        for copy in weight_copies(expert, expert - 1):
            copy.start()
    reset_base()
    relay_meta(far, None, right)
    for j in range(split, nz):
        wait_sib_tables(j)
    lax.fori_loop(split, nz, slot_tables, 0)
    for side in range(2):
        for i in range(3):
            far_copy(side, i).wait_recv()
    expert_pass(split, nz, split, True, lambda l: None, range(nz - 1, split - 1, -1))

    for m in range(cuts):
        for j in range(split):
            for c in range(2):
                if (j, c) != (0, 0):
                    ret_copy(j, c, m).wait_recv()
    for m in range(cuts):
        for j in range(split, nz):
            for c in range(2):
                ret_copy(j, c, m).wait_recv()
        n = m * nt
        moe_sum = dot_tn(comb[...], ret[:, n:n + nt])
        out[:, n:n + nt] = (xall[0, 0:tok_dev, n:n + nt].astype(F32) + moe_sum).astype(BF16)

    for side in range(2):
        for i in range(3):
            far_copy(side, i).wait_send()
    for j in range(nz):
        for i in range(2):
            msib_copy(i, j).wait_send()
            if j > 0:
                mring_copy(i, 0, j, right).wait_send()
        if j < split:
            for sub in range(SUBS):
                sib_copy(tok.at[sub_ds(sub)], j, sub).wait_send()
                if j > 0:
                    ring_copy(tok.at[sub_ds(sub)], j, sub, right).wait_send()
        for c in range(2):
            for m in range(cuts):
                if (j, c) != (0, 0):
                    ret_copy(j, c, m).wait_send()


def solution(mesh):
    groups = mesh.shape['ep']
    nz = groups // 2
    row_spec = P(('dp', 'ep'))
    expert_spec = P('ep')

    def device_step(tokens, expert_ids, gate_vals, w_gate, w_up, w_down):
        tok_dev, top_k = expert_ids.shape
        d_model = tokens.shape[1]
        local, _, ffn = w_gate.shape
        cap = tok_dev * (top_k // 2) // groups
        ecap = tok_dev * top_k // local
        row_count = groups * cap
        most = (2 * (nz // 2) - 3) * 2 * cap
        hbm = pl.BlockSpec(memory_space=pl.ANY)
        dma = pltpu.SemaphoreType.DMA
        return pl.pallas_call(
            functools.partial(moe_kernel, groups),
            out_shape=jax.ShapeDtypeStruct(tokens.shape, tokens.dtype),
            in_specs=[hbm] * 6,
            out_specs=pl.BlockSpec(memory_space=pltpu.VMEM),
            scratch_shapes=[
                pltpu.VMEM((2 * (nz // 2) - 3, 2 * tok_dev, d_model), BF16),
                pltpu.VMEM((nz, top_k, 2 * tok_dev), jnp.int32),
                pltpu.VMEM((nz, top_k, 2 * tok_dev), F32),
                pltpu.VMEM((row_count, d_model), BF16),
                pltpu.VMEM((most, d_model // 4), F32),
                pltpu.VMEM((row_count, d_model), BF16),
                pltpu.VMEM((3, d_model, ffn), BF16),
                pltpu.VMEM((3, d_model, ffn), BF16),
                pltpu.VMEM((2, ffn, d_model), BF16),
                pltpu.VMEM((local, ecap, d_model), BF16),
                pltpu.VMEM((local, ecap, ffn), BF16),
                pltpu.VMEM((ecap, most), BF16),
                pltpu.VMEM((local, most, ecap), BF16),
                pltpu.VMEM((local, row_count), F32),
                pltpu.VMEM((row_count, local), F32),
                pltpu.VMEM((row_count, local), F32),
                pltpu.VMEM((row_count, tok_dev), BF16),
                pltpu.VMEM((tok_dev, tok_dev), BF16),
                pltpu.VMEM((local, 1), F32),
                pltpu.VMEM((1, local), F32),
                pltpu.VMEM((3, 2 * cap, 2 * tok_dev), BF16),
                pltpu.VMEM((2, 3 * cap, tok_dev), BF16),
                pltpu.VMEM((2, 3 * cap, d_model), BF16),
                dma((nz, SUBS)), dma((nz, SUBS)), dma((nz, SUBS)), dma((nz, SUBS)),
                dma((nz, 2)), dma((nz, 2)), dma((nz, 2)), dma((nz, 2)),
                dma((2, 3)), dma((2, 3)), dma((nz, 2, 4)), dma((nz, 2, 4)), dma((3, 2)), dma((2, local)), dma((3,)),
            ],
            compiler_params=pltpu.CompilerParams(collective_id=0, has_side_effects=True, vmem_limit_bytes=67043328),
            name='moe_fused',
        )(tokens, expert_ids.T, gate_vals.T, w_gate, w_up, w_down)

    return jax.shard_map(device_step, mesh=mesh, in_specs=(row_spec, row_spec, row_spec, expert_spec, expert_spec, expert_spec), out_specs=row_spec, check_vma=False)
```

```python
import functools

import jax
import jax.numpy as jnp
from jax import lax
from jax.experimental import pallas as pl
from jax.experimental.pallas import tpu as pltpu
from jax.sharding import PartitionSpec as P

MESH = pl.DeviceIdType.MESH
SUBS = 4
F32 = jnp.float32
BF16 = jnp.bfloat16


def dot(a, b):
    return jnp.dot(a, b, preferred_element_type=F32)


def dot_nt(a, b, precision=None):
    return lax.dot_general(a, b, (((1,), (1,)), ((), ())), precision=precision, preferred_element_type=F32)


def dot_tn(a, b):
    return lax.dot_general(a, b, (((0,), (0,)), ((), ())), preferred_element_type=F32)


def moe_kernel(groups, tok, ids_in, gates_in, w_gate, w_up, w_down, ret, comb_out, xall, ids_all, gates_all, rows, acc, wgb, wub, wdb, xin, hid, fan, fan_t,
               slot_r, slot_c, gate_c, comb, tri, base_r, base_c, packs, ship, sends, ring_s, ring_r, sib_s, sib_r, mring_s, mring_r, msib_s, msib_r,
               far_s, far_r, ret_s, ret_r, wsem, dsem, loc):
    nz = groups // 2
    half = nz // 2
    tok_dev, d_model = tok.shape
    local, _, ffn = w_gate.shape
    top_k = ids_in.shape[0]
    cap = tok_dev * (top_k // 2) // groups
    ecap = fan.shape[0]
    sub_rows = tok_dev // SUBS
    blk = 2 * cap
    cuts = 4
    nt = d_model // cuts
    ft = min(256, ffn)
    far = nz - 1
    split = 2 * half - 3

    me = lax.axis_index('ep')
    z = me // 2
    k = me % 2
    right = ((z + 1) % nz) * 2 + k
    left = ((z + nz - 1) % nz) * 2 + k
    sib = z * 2 + 1 - k

    def source_shift(j):
        if j == 0:
            return 0
        if j == far:
            return half
        return nz - (j + 1) // 2 if j % 2 == 1 else j // 2

    def device_at(shift, c):
        return ((z + shift) % nz) * 2 + (k if c == 0 else 1 - k)

    def remote(src, dst, ssem, rsem, dev):
        return pltpu.make_async_remote_copy(src_ref=src, dst_ref=dst, send_sem=ssem, recv_sem=rsem, device_id={'ep': dev}, device_id_type=MESH)

    def sub_ds(sub, c=0):
        return pl.ds(c * tok_dev + sub * sub_rows, sub_rows)

    def swing(i):
        return (i + SUBS // 2) % SUBS

    def ring_copy(src, dst_j, sub, dev):
        return remote(src, xall.at[dst_j, sub_ds(sub)], ring_s.at[dst_j, sub], ring_r.at[dst_j, sub], dev)

    def sib_copy(src, j, sub):
        return remote(src, xall.at[j, sub_ds(sub, 1)], sib_s.at[j, sub], sib_r.at[j, sub], sib)

    tables = ((ids_in, ids_all), (gates_in, gates_all))

    def table_src(i, j, own):
        return tables[i][0] if own else tables[i][1].at[j, :, pl.ds(0, tok_dev)]

    def mring_copy(i, src_j, dst_j, dev):
        return remote(table_src(i, src_j, src_j == 0), tables[i][1].at[dst_j, :, pl.ds(0, tok_dev)], mring_s.at[dst_j, i], mring_r.at[dst_j, i], dev)

    def msib_copy(i, j):
        return remote(table_src(i, j, j == 0), tables[i][1].at[j, :, pl.ds(tok_dev, tok_dev)], msib_s.at[j, i], msib_r.at[j, i], sib)

    def columns(m):
        return pl.ds(pl.multiple_of(m * nt, nt), nt)

    def ret_copy(j, c, m):
        part = (pl.ds(j * blk + c * cap, cap), columns(m))
        return remote(rows.at[part], ret.at[part], ret_s.at[j, c, m], ret_r.at[j, c, m], device_at(source_shift(j), c))

    def self_copy(m):
        part = (pl.ds(0, cap), columns(m))
        return pltpu.make_async_copy(rows.at[part], ret.at[part], ret_s.at[0, 0, m])

    comb_copy = pltpu.make_async_copy(comb, comb_out, loc.at[3])

    def far_copy(side, i):
        j, c = ((split, 0), (split, 1), (far, 0))[i] if side == 0 else ((split + 1, 0), (split + 1, 1), (far, 1))[i]
        shift = (1, 1, 2)[i] if side == 0 else (nz - 1, nz - 1, nz - 2)[i]
        core = (0, 1, side)[i]
        src = sends.at[side, pl.ds(i * cap, cap)]
        return remote(src, rows.at[pl.ds(j * blk + c * cap, cap)], far_s.at[side, i], far_r.at[side, i], device_at(shift, core))

    def weight_copies(expert, slot):
        return (pltpu.make_async_copy(w_gate.at[expert], wgb.at[slot], wsem.at[slot, 0]),
                pltpu.make_async_copy(w_up.at[expert], wub.at[slot], wsem.at[slot, 1]))

    def down_tile(l, bank):
        if bank == 0:
            return wdb.at[l // 4, :, pl.ds((l % 4) * nt, nt)]
        buf = wgb if l < 4 else wub
        return buf.at[(l % 4) // 2, pl.ds((l % 2) * ffn, ffn), pl.ds(0, nt)]

    def down_copies(m, bank):
        return [pltpu.make_async_copy(w_down.at[l, :, columns(m)], down_tile(l, bank), dsem.at[bank, l]) for l in range(local)]

    own_tok = pltpu.make_async_copy(tok, xall.at[0, pl.ds(0, tok_dev)], loc.at[0])
    own_tables = [pltpu.make_async_copy(tables[i][0], tables[i][1].at[0, :, pl.ds(0, tok_dev)], loc.at[1 + i]) for i in range(2)]
    for copy in own_tables:
        copy.start()
    own_tok.start()

    barrier = pltpu.get_barrier_semaphore()
    for peer in (right, left, sib):
        pl.semaphore_signal(barrier, inc=1, device_id={'ep': peer}, device_id_type=MESH)
    pl.semaphore_wait(barrier, 3)

    for i in range(2):
        mring_copy(i, 0, 1, right).start()
        mring_copy(i, 0, 2, left).start()
        msib_copy(i, 0).start()
    for i in range(SUBS):
        ring_copy(tok.at[sub_ds(i)], 1, i, right).start()
        ring_copy(tok.at[sub_ds(swing(i))], 2, swing(i), left).start()
    for sub in range(SUBS):
        sib_copy(tok.at[sub_ds(sub)], 0, sub).start()
    for expert in range(3):
        for copy in weight_copies(expert, (expert + 2) % 3):
            copy.start()

    def relay_meta(j, next_j, dev):
        for i in range(2):
            mring_copy(i, j, j, dev).wait_recv()
            if next_j is not None:
                mring_copy(i, j, next_j, dev).start()
            msib_copy(i, j).start()

    def relay_sub(j, sub, next_j, dev):
        here = xall.at[j, sub_ds(sub)]
        ring_copy(here, j, sub, dev).wait_recv()
        if next_j is not None:
            ring_copy(here, next_j, sub, dev).start()
        sib_copy(here, j, sub).start()

    def wait_sib_tables(j):
        for i in range(2):
            msib_copy(i, j).wait_recv()

    def wait_sib(j):
        for sub in range(SUBS):
            sib_copy(xall.at[j, sub_ds(sub)], j, sub).wait_recv()

    tok_row = lax.broadcasted_iota(jnp.int32, (tok_dev, tok_dev), 0)
    tok_col = lax.broadcasted_iota(jnp.int32, (tok_dev, tok_dev), 1)
    tri[...] = jnp.where(tok_row < tok_col, 1.0, 0.0).astype(BF16)

    for copy in own_tables:
        copy.wait()
    row_id = lax.broadcasted_iota(jnp.int32, (2 * nz, tok_dev), 0)
    peer_lo = jnp.zeros((2 * nz, tok_dev), jnp.int32)
    for j in range(nz):
        for c in range(2):
            peer = device_at((nz - source_shift(j)) % nz, c)
            peer_lo = jnp.where(row_id == 2 * j + c, peer * local, peer_lo)
    own_ids = ids_all[0, :, 0:tok_dev]
    picked = jnp.zeros((2 * nz, tok_dev), F32)
    for i in range(top_k):
        rel = own_ids[i:i + 1, :] - peer_lo
        picked = jnp.where((rel >= 0) & (rel < local), 1.0, picked)
    rank = jnp.where(picked > 0, dot(picked.astype(BF16), tri[...]), -1.0)
    cap_iota = lax.broadcasted_iota(jnp.int32, (cap, tok_dev), 0).astype(F32)
    for r in range(2 * nz):
        comb[r * cap:(r + 1) * cap, :] = jnp.where(rank[r:r + 1, :] == cap_iota, 1.0, 0.0).astype(BF16)

    comb_copy.start()
    lo = me * local

    def reset_base():
        base_r[...] = jnp.zeros_like(base_r)
        base_c[...] = jnp.zeros_like(base_c)

    def slot_tables(j, carry):
        gts = gates_all[j]
        rel = ids_all[j] - lo
        chosen = jnp.max(jnp.where((rel >= 0) & (rel < local), 1.0, 0.0), axis=0, keepdims=True)
        halves = []
        for c in range(2):
            ch = jnp.broadcast_to(chosen[:, c * tok_dev:(c + 1) * tok_dev], (8, tok_dev)).astype(BF16)
            halves.append(dot(ch, tri[...])[0:1, :] + float(c * cap))
        rank2 = jnp.where(chosen > 0, jnp.concatenate(halves, axis=1), -1.0)
        pack = jnp.where(rank2 == lax.broadcasted_iota(jnp.int32, (blk, 2 * tok_dev), 0).astype(F32), 1.0, 0.0)
        pack_b = pack.astype(BF16)
        loc_iota = lax.broadcasted_iota(jnp.int32, (local, 2 * tok_dev), 0)
        mem = jnp.zeros((local, 2 * tok_dev), F32)
        gat = jnp.zeros((local, 2 * tok_dev), F32)
        for i in range(top_k):
            hit = rel[i:i + 1, :] == loc_iota
            mem = jnp.where(hit, 1.0, mem)
            gat = jnp.where(hit, gts[i:i + 1, :], gat)
        mem_b = mem.astype(BF16)
        mem_r = dot_nt(mem_b, pack_b)
        mem_c = dot_nt(pack_b, mem_b)
        gate_j = dot_nt(pack, gat, lax.Precision.HIGHEST)
        tri_b = tri[0:blk, 0:blk]
        pos_r = dot(mem_r.astype(BF16), tri_b) + base_r[...]
        pos_c = dot_tn(tri_b, mem_c.astype(BF16)) + base_c[...]
        here = pl.ds(pl.multiple_of(j * blk, blk), blk)
        slot_r[:, here] = jnp.where(mem_r > 0, pos_r, -1.0)
        slot_c[here, :] = jnp.where(mem_c > 0, pos_c, -1.0)
        gate_c[here, :] = gate_j
        base_r[...] += jnp.sum(mem_r, axis=1, keepdims=True)
        base_c[...] += jnp.sum(mem_c, axis=0, keepdims=True)

        packs[j % 3] = pack_b
        return carry

    def pack_rows(j, carry):
        here = pl.ds(pl.multiple_of(j * blk, blk), blk)
        for n in range(0, d_model, nt):
            rows[here, n:n + nt] = dot(packs[j % 3], xall[j, :, n:n + nt]).astype(BF16)
        return carry

    def gather(l, a, b, add):
        lo_r, hi_r = a * blk, b * blk
        wide = hi_r - lo_r
        row_pos = slot_r[pl.ds(l, 1), lo_r:hi_r]
        fan[:, 0:wide] = jnp.where(row_pos == lax.broadcasted_iota(jnp.int32, (ecap, wide), 0).astype(F32), 1.0, 0.0).astype(BF16)
        for n in range(0, d_model, nt):
            got = dot(fan[:, 0:wide], rows[lo_r:hi_r, n:n + nt])
            if add:
                got = got + xin[l, :, n:n + nt].astype(F32)
            xin[l, :, n:n + nt] = got.astype(BF16)

    def expert_pass(j0, j1, g0, last, hook, order):
        r0, count = j0 * blk, (j1 - j0) * blk
        for copy in down_copies(0, 0):
            copy.start()
        gather(0, g0, j1, g0 != j0)

        def expert(l, carry):
            slot = (l + 2) % 3
            hook(l)

            def prefetch():
                for copy in weight_copies(l + 2, (l + 1) % 3):
                    copy.start()

            def prefetch_next_pass():
                for copy in weight_copies(0, 2):
                    copy.start()

            pl.when((l > 0) & (l < local - 2))(prefetch)
            if not last:
                pl.when(l == local - 1)(prefetch_next_pass)
            for copy in weight_copies(l, slot):
                copy.wait()
            for f in range(0, ffn, ft):
                gate_act = dot(xin[l], wgb[slot, :, f:f + ft])
                up_act = dot(xin[l], wub[slot, :, f:f + ft])
                hid[l, :, f:f + ft] = (jax.nn.silu(gate_act) * up_act).astype(BF16)
            gather((l + 1) % local, g0, j1, g0 != j0)
            lane = lax.broadcasted_iota(jnp.int32, (count, local), 1) == l
            pos = jnp.sum(jnp.where(lane, slot_c[r0:r0 + count, :], 0.0), axis=1, keepdims=True)
            fan_t[l, 0:count, :] = jnp.where(pos == lax.broadcasted_iota(jnp.int32, (count, ecap), 1).astype(F32), 1.0, 0.0).astype(BF16)
            return carry

        lax.fori_loop(0, local, expert, 0)

        def column(m, bank):
            for copy in down_copies(m, bank):
                copy.wait()

            def spread(l, y):
                part = gate_c[r0:r0 + count, l:l + 1] * dot(fan_t[l, 0:count, :], y)
                if l == 0:
                    acc[0:count, :] = part
                else:
                    acc[0:count, :] += part

            held = None
            for l in range(local):
                tile = wdb[l // 4, :, (l % 4) * nt:(l % 4 + 1) * nt] if bank == 0 else (wgb if l < 4 else wub)[(l % 4) // 2, (l % 2) * ffn:(l % 2 + 1) * ffn, 0:nt]
                y = dot(hid[l], tile).astype(BF16)
                if held is not None:
                    spread(*held)
                held = (l, y)
            spread(*held)
            rows[r0:r0 + count, columns(m)] = acc[0:count, :].astype(BF16)
            if j0 == 0:
                self_copy(m).start()
            for j in order:
                for c in range(2):
                    if (j, c) != (0, 0):
                        ret_copy(j, c, m).start()

        def two_columns(i, carry):
            for copy in down_copies(2 * i + 1, 1):
                copy.start()
            column(2 * i, 0)

            def prefetch():
                for copy in down_copies(2 * i + 2, 0):
                    copy.start()

            pl.when(i < cuts // 2 - 1)(prefetch)
            column(2 * i + 1, 1)
            return carry

        lax.fori_loop(0, cuts // 2, two_columns, 0)

    def ship_tables(side, j):
        ids = ids_all[j, :, 0:tok_dev]
        row_id = lax.broadcasted_iota(jnp.int32, (8, tok_dev), 0)
        peers = [device_at(shift, core) for shift, core in (((1, 0), (1, 1), (2, 0)) if side == 0 else ((nz - 1, 0), (nz - 1, 1), (nz - 2, 1)))]
        low = jnp.full((8, tok_dev), groups * local, jnp.int32)
        for i, peer in enumerate(peers):
            low = jnp.where(row_id == i, peer * local, low)
        took = jnp.zeros((8, tok_dev), F32)
        for i in range(top_k):
            rel = ids[i:i + 1, :] - low
            took = jnp.where((rel >= 0) & (rel < local), 1.0, took)
        place = jnp.where(took > 0, dot(took.astype(BF16), tri[...]), -1.0)
        for i in range(3):
            ship[side, i * cap:(i + 1) * cap, :] = jnp.where(place[i:i + 1, :] == cap_iota, 1.0, 0.0).astype(BF16)

    def ship_rows(side, j):
        for n in range(0, d_model, nt):
            sends[side, :, n:n + nt] = dot(ship[side], xall[j, 0:tok_dev, n:n + nt]).astype(BF16)
        for i in range(3):
            far_copy(side, i).start()

    reset_base()
    wait_sib_tables(0)
    lax.fori_loop(0, 1, slot_tables, 0)
    own_tok.wait()
    wait_sib(0)
    lax.fori_loop(0, 1, pack_rows, 0)
    for s in range(1, half - 1):
        jr, jl = 2 * s - 1, 2 * s
        relay_meta(jr, jr + 2, right)
        relay_meta(jl, jl + 2, left)
        wait_sib_tables(jr)
        wait_sib_tables(jl)
        lax.fori_loop(jr, jl + 1, slot_tables, 0)
        onward = s < half - 2
        if not onward:
            ship_tables(0, jr)
            ship_tables(1, jl)
        for i in range(SUBS):
            relay_sub(jr, i, jr + 2 if onward else None, right)
            relay_sub(jl, swing(i), jl + 2 if onward else None, left)
        if not onward:
            ship_rows(0, jr)
            ship_rows(1, jl)
        wait_sib(jr)
        wait_sib(jl)
        lax.fori_loop(jr, jl + 1, pack_rows, 0)
        if s == half - 3:
            def early(l, carry):
                gather(l, 0, jl + 1, False)
                return carry

            lax.fori_loop(0, local, early, 0)
            reached = jl + 1

    jr, jl = split, split + 1

    def hook_a(l):
        def meta_step():
            relay_meta(jr, far, right)
            relay_meta(jl, None, left)

        pl.when(l == 0)(meta_step)

    expert_pass(0, split, reached, False, hook_a, range(split - 1, -1, -1))
    for expert in (1, 2):
        for copy in weight_copies(expert, expert - 1):
            copy.start()
    reset_base()
    relay_meta(far, None, right)
    for j in range(split, nz):
        wait_sib_tables(j)
    lax.fori_loop(split, nz, slot_tables, 0)
    for side in range(2):
        for i in range(3):
            far_copy(side, i).wait_recv()
    expert_pass(split, nz, split, True, lambda l: None, range(nz - 1, split - 1, -1))

    for m in range(cuts):
        for j in range(split):
            for c in range(2):
                if (j, c) != (0, 0):
                    ret_copy(j, c, m).wait_recv()
    for m in range(cuts):
        for j in range(split, nz):
            for c in range(2):
                ret_copy(j, c, m).wait_recv()
        self_copy(m).wait()
    comb_copy.wait()

    for side in range(2):
        for i in range(3):
            far_copy(side, i).wait_send()
    for j in range(nz):
        for i in range(2):
            msib_copy(i, j).wait_send()
            if j > 0:
                mring_copy(i, 0, j, right).wait_send()
        if j < split:
            for sub in range(SUBS):
                sib_copy(tok.at[sub_ds(sub)], j, sub).wait_send()
                if j > 0:
                    ring_copy(tok.at[sub_ds(sub)], j, sub, right).wait_send()
        for c in range(2):
            for m in range(cuts):
                if (j, c) != (0, 0):
                    ret_copy(j, c, m).wait_send()


def solution(mesh):
    groups = mesh.shape['ep']
    nz = groups // 2
    row_spec = P(('dp', 'ep'))
    expert_spec = P('ep')

    def device_step(tokens, expert_ids, gate_vals, w_gate, w_up, w_down):
        tok_dev, top_k = expert_ids.shape
        d_model = tokens.shape[1]
        local, _, ffn = w_gate.shape
        cap = tok_dev * (top_k // 2) // groups
        ecap = tok_dev * top_k // local
        row_count = groups * cap
        most = (2 * (nz // 2) - 3) * 2 * cap
        hbm = pl.BlockSpec(memory_space=pl.ANY)
        dma = pltpu.SemaphoreType.DMA
        returned, comb = pl.pallas_call(
            functools.partial(moe_kernel, groups),
            out_shape=[jax.ShapeDtypeStruct((row_count, d_model), BF16), jax.ShapeDtypeStruct((row_count, tok_dev), BF16)],
            in_specs=[hbm] * 6,
            out_specs=[hbm] * 2,
            scratch_shapes=[
                pltpu.VMEM((2 * (nz // 2) - 3, 2 * tok_dev, d_model), BF16),
                pltpu.VMEM((nz, top_k, 2 * tok_dev), jnp.int32),
                pltpu.VMEM((nz, top_k, 2 * tok_dev), F32),
                pltpu.VMEM((row_count, d_model), BF16),
                pltpu.VMEM((most, d_model // 4), F32),
                pltpu.VMEM((3, d_model, ffn), BF16),
                pltpu.VMEM((3, d_model, ffn), BF16),
                pltpu.VMEM((2, ffn, d_model), BF16),
                pltpu.VMEM((local, ecap, d_model), BF16),
                pltpu.VMEM((local, ecap, ffn), BF16),
                pltpu.VMEM((ecap, most), BF16),
                pltpu.VMEM((local, most, ecap), BF16),
                pltpu.VMEM((local, row_count), F32),
                pltpu.VMEM((row_count, local), F32),
                pltpu.VMEM((row_count, local), F32),
                pltpu.VMEM((row_count, tok_dev), BF16),
                pltpu.VMEM((tok_dev, tok_dev), BF16),
                pltpu.VMEM((local, 1), F32),
                pltpu.VMEM((1, local), F32),
                pltpu.VMEM((3, 2 * cap, 2 * tok_dev), BF16),
                pltpu.VMEM((2, 3 * cap, tok_dev), BF16),
                pltpu.VMEM((2, 3 * cap, d_model), BF16),
                dma((nz, SUBS)), dma((nz, SUBS)), dma((nz, SUBS)), dma((nz, SUBS)),
                dma((nz, 2)), dma((nz, 2)), dma((nz, 2)), dma((nz, 2)),
                dma((2, 3)), dma((2, 3)), dma((nz, 2, 4)), dma((nz, 2, 4)), dma((3, 2)), dma((2, local)), dma((4,)),
            ],
            compiler_params=pltpu.CompilerParams(collective_id=0, has_side_effects=True, vmem_limit_bytes=67043328),
            name='moe_fused',
        )(tokens, expert_ids.T, gate_vals.T, w_gate, w_up, w_down)
        return (tokens.astype(F32) + dot_tn(comb, returned)).astype(BF16)

    return jax.shard_map(device_step, mesh=mesh, in_specs=(row_spec, row_spec, row_spec, expert_spec, expert_spec, expert_spec), out_specs=row_spec, check_vma=False)
```

```python
import functools

import jax
import jax.numpy as jnp
from jax import lax
from jax.experimental import pallas as pl
from jax.experimental.pallas import tpu as pltpu
from jax.sharding import PartitionSpec as P

MESH = pl.DeviceIdType.MESH
SUBS = 4
F32 = jnp.float32
BF16 = jnp.bfloat16


def dot(a, b):
    return jnp.dot(a, b, preferred_element_type=F32)


def dot_nt(a, b, precision=None):
    return lax.dot_general(a, b, (((1,), (1,)), ((), ())), precision=precision, preferred_element_type=F32)


def dot_tn(a, b):
    return lax.dot_general(a, b, (((0,), (0,)), ((), ())), preferred_element_type=F32)


def moe_kernel(groups, tok, ids_in, gates_in, w_gate, w_up, w_down, out, xall, ids_all, gates_all, rows, acc, ret, wgb, wub, wdb, xin, hid, fan, fan_t,
               slot_r, slot_c, gate_c, comb, tri, base_r, base_c, packs, ship, sends, ring_s, ring_r, sib_s, sib_r, mring_s, mring_r, msib_s, msib_r,
               far_s, far_r, ret_s, ret_r, wsem, dsem, loc, out_buf, out_sem):
    nz = groups // 2
    half = nz // 2
    tok_dev, d_model = tok.shape
    local, _, ffn = w_gate.shape
    top_k = ids_in.shape[0]
    cap = tok_dev * (top_k // 2) // groups
    ecap = fan.shape[0]
    sub_rows = tok_dev // SUBS
    blk = 2 * cap
    cuts = 4
    nt = d_model // cuts
    ft = min(256, ffn)
    far = nz - 1
    split = 2 * half - 3

    me = lax.axis_index('ep')
    z = me // 2
    k = me % 2
    right = ((z + 1) % nz) * 2 + k
    left = ((z + nz - 1) % nz) * 2 + k
    sib = z * 2 + 1 - k

    def source_shift(j):
        if j == 0:
            return 0
        if j == far:
            return half
        return nz - (j + 1) // 2 if j % 2 == 1 else j // 2

    def device_at(shift, c):
        return ((z + shift) % nz) * 2 + (k if c == 0 else 1 - k)

    def remote(src, dst, ssem, rsem, dev):
        return pltpu.make_async_remote_copy(src_ref=src, dst_ref=dst, send_sem=ssem, recv_sem=rsem, device_id={'ep': dev}, device_id_type=MESH)

    def sub_ds(sub, c=0):
        return pl.ds(c * tok_dev + sub * sub_rows, sub_rows)

    def swing(i):
        return (i + SUBS // 2) % SUBS

    def ring_copy(src, dst_j, sub, dev):
        return remote(src, xall.at[dst_j, sub_ds(sub)], ring_s.at[dst_j, sub], ring_r.at[dst_j, sub], dev)

    def sib_copy(src, j, sub):
        return remote(src, xall.at[j, sub_ds(sub, 1)], sib_s.at[j, sub], sib_r.at[j, sub], sib)

    tables = ((ids_in, ids_all), (gates_in, gates_all))

    def table_src(i, j, own):
        return tables[i][0] if own else tables[i][1].at[j, :, pl.ds(0, tok_dev)]

    def mring_copy(i, src_j, dst_j, dev):
        return remote(table_src(i, src_j, src_j == 0), tables[i][1].at[dst_j, :, pl.ds(0, tok_dev)], mring_s.at[dst_j, i], mring_r.at[dst_j, i], dev)

    def msib_copy(i, j):
        return remote(table_src(i, j, j == 0), tables[i][1].at[j, :, pl.ds(tok_dev, tok_dev)], msib_s.at[j, i], msib_r.at[j, i], sib)

    def columns(m):
        return pl.ds(pl.multiple_of(m * nt, nt), nt)

    def ret_copy(j, c, m):
        part = (pl.ds(j * blk + c * cap, cap), columns(m))
        return remote(rows.at[part], ret.at[part], ret_s.at[j, c, m], ret_r.at[j, c, m], device_at(source_shift(j), c))

    def out_copy(m):
        return pltpu.make_async_copy(out_buf.at[:, columns(m)], out.at[:, columns(m)], out_sem.at[m])

    def far_copy(side, i):
        j, c = ((split, 0), (split, 1), (far, 0))[i] if side == 0 else ((split + 1, 0), (split + 1, 1), (far, 1))[i]
        shift = (1, 1, 2)[i] if side == 0 else (nz - 1, nz - 1, nz - 2)[i]
        core = (0, 1, side)[i]
        src = sends.at[side, pl.ds(i * cap, cap)]
        return remote(src, rows.at[pl.ds(j * blk + c * cap, cap)], far_s.at[side, i], far_r.at[side, i], device_at(shift, core))

    def weight_copies(expert, slot):
        return (pltpu.make_async_copy(w_gate.at[expert], wgb.at[slot], wsem.at[slot, 0]),
                pltpu.make_async_copy(w_up.at[expert], wub.at[slot], wsem.at[slot, 1]))

    def down_tile(l, bank):
        if bank == 0:
            return wdb.at[l // 4, :, pl.ds((l % 4) * nt, nt)]
        buf = wgb if l < 4 else wub
        return buf.at[(l % 4) // 2, pl.ds((l % 2) * ffn, ffn), pl.ds(0, nt)]

    def down_copies(m, bank):
        return [pltpu.make_async_copy(w_down.at[l, :, columns(m)], down_tile(l, bank), dsem.at[bank, l]) for l in range(local)]

    own_tok = pltpu.make_async_copy(tok, xall.at[0, pl.ds(0, tok_dev)], loc.at[0])
    own_tables = [pltpu.make_async_copy(tables[i][0], tables[i][1].at[0, :, pl.ds(0, tok_dev)], loc.at[1 + i]) for i in range(2)]
    for copy in own_tables:
        copy.start()
    own_tok.start()

    barrier = pltpu.get_barrier_semaphore()
    for peer in (right, left, sib):
        pl.semaphore_signal(barrier, inc=1, device_id={'ep': peer}, device_id_type=MESH)
    pl.semaphore_wait(barrier, 3)

    for i in range(2):
        mring_copy(i, 0, 1, right).start()
        mring_copy(i, 0, 2, left).start()
        msib_copy(i, 0).start()
    for i in range(SUBS):
        ring_copy(tok.at[sub_ds(i)], 1, i, right).start()
        ring_copy(tok.at[sub_ds(swing(i))], 2, swing(i), left).start()
    for sub in range(SUBS):
        sib_copy(tok.at[sub_ds(sub)], 0, sub).start()
    for expert in range(3):
        for copy in weight_copies(expert, (expert + 2) % 3):
            copy.start()

    def relay_meta(j, next_j, dev):
        for i in range(2):
            mring_copy(i, j, j, dev).wait_recv()
            if next_j is not None:
                mring_copy(i, j, next_j, dev).start()
            msib_copy(i, j).start()

    def relay_sub(j, sub, next_j, dev):
        here = xall.at[j, sub_ds(sub)]
        ring_copy(here, j, sub, dev).wait_recv()
        if next_j is not None:
            ring_copy(here, next_j, sub, dev).start()
        sib_copy(here, j, sub).start()

    def wait_sib_tables(j):
        for i in range(2):
            msib_copy(i, j).wait_recv()

    def wait_sib(j):
        for sub in range(SUBS):
            sib_copy(xall.at[j, sub_ds(sub)], j, sub).wait_recv()

    tok_row = lax.broadcasted_iota(jnp.int32, (tok_dev, tok_dev), 0)
    tok_col = lax.broadcasted_iota(jnp.int32, (tok_dev, tok_dev), 1)
    tri[...] = jnp.where(tok_row < tok_col, 1.0, 0.0).astype(BF16)

    for copy in own_tables:
        copy.wait()
    row_id = lax.broadcasted_iota(jnp.int32, (2 * nz, tok_dev), 0)
    peer_lo = jnp.zeros((2 * nz, tok_dev), jnp.int32)
    for j in range(nz):
        for c in range(2):
            peer = device_at((nz - source_shift(j)) % nz, c)
            peer_lo = jnp.where(row_id == 2 * j + c, peer * local, peer_lo)
    own_ids = ids_all[0, :, 0:tok_dev]
    picked = jnp.zeros((2 * nz, tok_dev), F32)
    for i in range(top_k):
        rel = own_ids[i:i + 1, :] - peer_lo
        picked = jnp.where((rel >= 0) & (rel < local), 1.0, picked)
    rank = jnp.where(picked > 0, dot(picked.astype(BF16), tri[...]), -1.0)
    cap_iota = lax.broadcasted_iota(jnp.int32, (cap, tok_dev), 0).astype(F32)
    for r in range(2 * nz):
        comb[r * cap:(r + 1) * cap, :] = jnp.where(rank[r:r + 1, :] == cap_iota, 1.0, 0.0).astype(BF16)

    lo = me * local

    def reset_base():
        base_r[...] = jnp.zeros_like(base_r)
        base_c[...] = jnp.zeros_like(base_c)

    def slot_tables(j, carry):
        gts = gates_all[j]
        rel = ids_all[j] - lo
        chosen = jnp.max(jnp.where((rel >= 0) & (rel < local), 1.0, 0.0), axis=0, keepdims=True)
        halves = []
        for c in range(2):
            ch = jnp.broadcast_to(chosen[:, c * tok_dev:(c + 1) * tok_dev], (8, tok_dev)).astype(BF16)
            halves.append(dot(ch, tri[...])[0:1, :] + float(c * cap))
        rank2 = jnp.where(chosen > 0, jnp.concatenate(halves, axis=1), -1.0)
        pack = jnp.where(rank2 == lax.broadcasted_iota(jnp.int32, (blk, 2 * tok_dev), 0).astype(F32), 1.0, 0.0)
        pack_b = pack.astype(BF16)
        loc_iota = lax.broadcasted_iota(jnp.int32, (local, 2 * tok_dev), 0)
        mem = jnp.zeros((local, 2 * tok_dev), F32)
        gat = jnp.zeros((local, 2 * tok_dev), F32)
        for i in range(top_k):
            hit = rel[i:i + 1, :] == loc_iota
            mem = jnp.where(hit, 1.0, mem)
            gat = jnp.where(hit, gts[i:i + 1, :], gat)
        mem_b = mem.astype(BF16)
        mem_r = dot_nt(mem_b, pack_b)
        mem_c = dot_nt(pack_b, mem_b)
        gate_j = dot_nt(pack, gat, lax.Precision.HIGHEST)
        tri_b = tri[0:blk, 0:blk]
        pos_r = dot(mem_r.astype(BF16), tri_b) + base_r[...]
        pos_c = dot_tn(tri_b, mem_c.astype(BF16)) + base_c[...]
        here = pl.ds(pl.multiple_of(j * blk, blk), blk)
        slot_r[:, here] = jnp.where(mem_r > 0, pos_r, -1.0)
        slot_c[here, :] = jnp.where(mem_c > 0, pos_c, -1.0)
        gate_c[here, :] = gate_j
        base_r[...] += jnp.sum(mem_r, axis=1, keepdims=True)
        base_c[...] += jnp.sum(mem_c, axis=0, keepdims=True)

        packs[j % 3] = pack_b
        return carry

    def pack_rows(j, carry):
        here = pl.ds(pl.multiple_of(j * blk, blk), blk)
        for n in range(0, d_model, nt):
            rows[here, n:n + nt] = dot(packs[j % 3], xall[j, :, n:n + nt]).astype(BF16)
        return carry

    def gather(l, a, b, add):
        lo_r, hi_r = a * blk, b * blk
        wide = hi_r - lo_r
        row_pos = slot_r[pl.ds(l, 1), lo_r:hi_r]
        fan[:, 0:wide] = jnp.where(row_pos == lax.broadcasted_iota(jnp.int32, (ecap, wide), 0).astype(F32), 1.0, 0.0).astype(BF16)
        for n in range(0, d_model, nt):
            got = dot(fan[:, 0:wide], rows[lo_r:hi_r, n:n + nt])
            if add:
                got = got + xin[l, :, n:n + nt].astype(F32)
            xin[l, :, n:n + nt] = got.astype(BF16)

    def expert_pass(j0, j1, g0, last, hook, order):
        r0, count = j0 * blk, (j1 - j0) * blk
        for copy in down_copies(0, 0):
            copy.start()
        gather(0, g0, j1, g0 != j0)

        def expert(l, carry):
            slot = (l + 2) % 3
            hook(l)

            def prefetch():
                for copy in weight_copies(l + 2, (l + 1) % 3):
                    copy.start()

            def prefetch_next_pass():
                for copy in weight_copies(0, 2):
                    copy.start()

            pl.when((l > 0) & (l < local - 2))(prefetch)
            if not last:
                pl.when(l == local - 1)(prefetch_next_pass)
            for copy in weight_copies(l, slot):
                copy.wait()
            for f in range(0, ffn, ft):
                gate_act = dot(xin[l], wgb[slot, :, f:f + ft])
                up_act = dot(xin[l], wub[slot, :, f:f + ft])
                hid[l, :, f:f + ft] = (jax.nn.silu(gate_act) * up_act).astype(BF16)
            gather((l + 1) % local, g0, j1, g0 != j0)
            lane = lax.broadcasted_iota(jnp.int32, (count, local), 1) == l
            pos = jnp.sum(jnp.where(lane, slot_c[r0:r0 + count, :], 0.0), axis=1, keepdims=True)
            fan_t[l, 0:count, :] = jnp.where(pos == lax.broadcasted_iota(jnp.int32, (count, ecap), 1).astype(F32), 1.0, 0.0).astype(BF16)
            return carry

        lax.fori_loop(0, local, expert, 0)

        def column(m, bank):
            for copy in down_copies(m, bank):
                copy.wait()

            def spread(l, y):
                part = gate_c[r0:r0 + count, l:l + 1] * dot(fan_t[l, 0:count, :], y)
                if l == 0:
                    acc[0:count, :] = part
                else:
                    acc[0:count, :] += part

            held = None
            for l in range(local):
                tile = wdb[l // 4, :, (l % 4) * nt:(l % 4 + 1) * nt] if bank == 0 else (wgb if l < 4 else wub)[(l % 4) // 2, (l % 2) * ffn:(l % 2 + 1) * ffn, 0:nt]
                y = dot(hid[l], tile).astype(BF16)
                if held is not None:
                    spread(*held)
                held = (l, y)
            spread(*held)
            rows[r0:r0 + count, columns(m)] = acc[0:count, :].astype(BF16)
            if j0 == 0:
                ret[0:cap, columns(m)] = acc[0:cap, :].astype(BF16)
            for j in order:
                for c in range(2):
                    if (j, c) != (0, 0):
                        ret_copy(j, c, m).start()

        def two_columns(i, carry):
            for copy in down_copies(2 * i + 1, 1):
                copy.start()
            column(2 * i, 0)

            def prefetch():
                for copy in down_copies(2 * i + 2, 0):
                    copy.start()

            pl.when(i < cuts // 2 - 1)(prefetch)
            column(2 * i + 1, 1)
            return carry

        lax.fori_loop(0, cuts // 2, two_columns, 0)

    def ship_tables(side, j):
        ids = ids_all[j, :, 0:tok_dev]
        row_id = lax.broadcasted_iota(jnp.int32, (8, tok_dev), 0)
        peers = [device_at(shift, core) for shift, core in (((1, 0), (1, 1), (2, 0)) if side == 0 else ((nz - 1, 0), (nz - 1, 1), (nz - 2, 1)))]
        low = jnp.full((8, tok_dev), groups * local, jnp.int32)
        for i, peer in enumerate(peers):
            low = jnp.where(row_id == i, peer * local, low)
        took = jnp.zeros((8, tok_dev), F32)
        for i in range(top_k):
            rel = ids[i:i + 1, :] - low
            took = jnp.where((rel >= 0) & (rel < local), 1.0, took)
        place = jnp.where(took > 0, dot(took.astype(BF16), tri[...]), -1.0)
        for i in range(3):
            ship[side, i * cap:(i + 1) * cap, :] = jnp.where(place[i:i + 1, :] == cap_iota, 1.0, 0.0).astype(BF16)

    def ship_rows(side, j):
        for n in range(0, d_model, nt):
            sends[side, :, n:n + nt] = dot(ship[side], xall[j, 0:tok_dev, n:n + nt]).astype(BF16)
        for i in range(3):
            far_copy(side, i).start()

    reset_base()
    wait_sib_tables(0)
    lax.fori_loop(0, 1, slot_tables, 0)
    own_tok.wait()
    wait_sib(0)
    lax.fori_loop(0, 1, pack_rows, 0)
    for s in range(1, half - 1):
        jr, jl = 2 * s - 1, 2 * s
        relay_meta(jr, jr + 2, right)
        relay_meta(jl, jl + 2, left)
        wait_sib_tables(jr)
        wait_sib_tables(jl)
        lax.fori_loop(jr, jl + 1, slot_tables, 0)
        onward = s < half - 2
        if not onward:
            ship_tables(0, jr)
            ship_tables(1, jl)
        for i in range(SUBS):
            relay_sub(jr, i, jr + 2 if onward else None, right)
            relay_sub(jl, swing(i), jl + 2 if onward else None, left)
        if not onward:
            ship_rows(0, jr)
            ship_rows(1, jl)
        wait_sib(jr)
        wait_sib(jl)
        lax.fori_loop(jr, jl + 1, pack_rows, 0)
        if s == half - 3:
            def early(l, carry):
                gather(l, 0, jl + 1, False)
                return carry

            lax.fori_loop(0, local, early, 0)
            reached = jl + 1

    jr, jl = split, split + 1

    def hook_a(l):
        def meta_step():
            relay_meta(jr, far, right)
            relay_meta(jl, None, left)

        pl.when(l == 0)(meta_step)

    expert_pass(0, split, reached, False, hook_a, range(split - 1, -1, -1))
    for expert in (1, 2):
        for copy in weight_copies(expert, expert - 1):
            copy.start()
    reset_base()
    relay_meta(far, None, right)
    for j in range(split, nz):
        wait_sib_tables(j)
    lax.fori_loop(split, nz, slot_tables, 0)
    for side in range(2):
        for i in range(3):
            far_copy(side, i).wait_recv()
    expert_pass(split, nz, split, True, lambda l: None, range(nz - 1, split - 1, -1))

    for m in range(cuts):
        for j in range(split):
            for c in range(2):
                if (j, c) != (0, 0):
                    ret_copy(j, c, m).wait_recv()
    for m in range(cuts):
        for j in range(split, nz):
            for c in range(2):
                ret_copy(j, c, m).wait_recv()
        n = m * nt
        moe_sum = dot_tn(comb[...], ret[:, n:n + nt])
        out_buf[:, n:n + nt] = (xall[0, 0:tok_dev, n:n + nt].astype(F32) + moe_sum).astype(BF16)
        out_copy(m).start()

    for side in range(2):
        for i in range(3):
            far_copy(side, i).wait_send()
    for j in range(nz):
        for i in range(2):
            msib_copy(i, j).wait_send()
            if j > 0:
                mring_copy(i, 0, j, right).wait_send()
        if j < split:
            for sub in range(SUBS):
                sib_copy(tok.at[sub_ds(sub)], j, sub).wait_send()
                if j > 0:
                    ring_copy(tok.at[sub_ds(sub)], j, sub, right).wait_send()
        for c in range(2):
            for m in range(cuts):
                if (j, c) != (0, 0):
                    ret_copy(j, c, m).wait_send()
    for m in range(cuts):
        out_copy(m).wait()


def solution(mesh):
    groups = mesh.shape['ep']
    nz = groups // 2
    row_spec = P(('dp', 'ep'))
    expert_spec = P('ep')

    def device_step(tokens, expert_ids, gate_vals, w_gate, w_up, w_down):
        tok_dev, top_k = expert_ids.shape
        d_model = tokens.shape[1]
        local, _, ffn = w_gate.shape
        cap = tok_dev * (top_k // 2) // groups
        ecap = tok_dev * top_k // local
        row_count = groups * cap
        most = (2 * (nz // 2) - 3) * 2 * cap
        hbm = pl.BlockSpec(memory_space=pl.ANY)
        dma = pltpu.SemaphoreType.DMA
        return pl.pallas_call(
            functools.partial(moe_kernel, groups),
            out_shape=jax.ShapeDtypeStruct(tokens.shape, tokens.dtype),
            in_specs=[hbm] * 6,
            out_specs=hbm,
            scratch_shapes=[
                pltpu.VMEM((2 * (nz // 2) - 3, 2 * tok_dev, d_model), BF16),
                pltpu.VMEM((nz, top_k, 2 * tok_dev), jnp.int32),
                pltpu.VMEM((nz, top_k, 2 * tok_dev), F32),
                pltpu.VMEM((row_count, d_model), BF16),
                pltpu.VMEM((most, d_model // 4), F32),
                pltpu.VMEM((row_count, d_model), BF16),
                pltpu.VMEM((3, d_model, ffn), BF16),
                pltpu.VMEM((3, d_model, ffn), BF16),
                pltpu.VMEM((2, ffn, d_model), BF16),
                pltpu.VMEM((local, ecap, d_model), BF16),
                pltpu.VMEM((local, ecap, ffn), BF16),
                pltpu.VMEM((ecap, most), BF16),
                pltpu.VMEM((local, most, ecap), BF16),
                pltpu.VMEM((local, row_count), F32),
                pltpu.VMEM((row_count, local), F32),
                pltpu.VMEM((row_count, local), F32),
                pltpu.VMEM((row_count, tok_dev), BF16),
                pltpu.VMEM((tok_dev, tok_dev), BF16),
                pltpu.VMEM((local, 1), F32),
                pltpu.VMEM((1, local), F32),
                pltpu.VMEM((3, 2 * cap, 2 * tok_dev), BF16),
                pltpu.VMEM((2, 3 * cap, tok_dev), BF16),
                pltpu.VMEM((2, 3 * cap, d_model), BF16),
                dma((nz, SUBS)), dma((nz, SUBS)), dma((nz, SUBS)), dma((nz, SUBS)),
                dma((nz, 2)), dma((nz, 2)), dma((nz, 2)), dma((nz, 2)),
                dma((2, 3)), dma((2, 3)), dma((nz, 2, 4)), dma((nz, 2, 4)), dma((3, 2)), dma((2, local)), dma((3,)),
                pltpu.VMEM((tok_dev, d_model), BF16), dma((4,)),
            ],
            compiler_params=pltpu.CompilerParams(collective_id=0, has_side_effects=True, vmem_limit_bytes=67043328),
            name='moe_fused',
        )(tokens, expert_ids.T, gate_vals.T, w_gate, w_up, w_down)

    return jax.shard_map(device_step, mesh=mesh, in_specs=(row_spec, row_spec, row_spec, expert_spec, expert_spec, expert_spec), out_specs=row_spec, check_vma=False)
```
